32 devices in a mesh: rep: 4 (over x, y), ep: 8 (over z, core).
Axes of the slice: x: 2, y: 2, z: 4, core: 2. Of those that a mesh axis runs over, the one named last changes fastest.
Arguments:
- x: bfloat16 [1024, 2048], P(('rep', 'ep')), parts along dimension 0
- cache: bfloat16 [1024, 256, 576], P(('rep', 'ep')), parts along dimension 0
- lens: int32 [1024], P(('rep', 'ep')), parts along dimension 0
- ids: int32 [1024, 6], P(('rep', 'ep')), parts along dimension 0
- rw: float32 [1024, 6], P(('rep', 'ep')), parts along dimension 0
- w_q: bfloat16 [2048, 3072], replicated
- w_dkv: bfloat16 [2048, 576], replicated
- w_uk: bfloat16 [16, 128, 512], replicated
- w_uv: bfloat16 [16, 512, 128], replicated
- w_o: bfloat16 [2048, 2048], replicated
- s_gate: bfloat16 [2048, 2816], replicated
- s_up: bfloat16 [2048, 2816], replicated
- s_down: bfloat16 [2816, 2048], replicated
- e_gate: bfloat16 [64, 2048, 1408], P('ep')
- e_up: bfloat16 [64, 2048, 1408], P('ep')
- e_down: bfloat16 [64, 1408, 2048], P('ep')
Outputs:
- output 1: bfloat16 [1024, 2048], P(('rep', 'ep')), parts along dimension 0
- output 2: bfloat16 [1024, 576], P(('rep', 'ep')), parts along dimension 0
There are 4 independent parts. The reference program is written for one: setup_inputs(seed, part) draws one part's arguments, and reference() takes and returns one part's arrays. A program takes and returns all parts, laid end to end along the dimension named above; an argument that names none is the same for every part.
All inputs are finite; a program needn't handle non-finite values.
Results may differ from the reference program's by a relative error of at most 0.0119281.
Values are sent between devices in bfloat16 or wider.
A program may use at most 1 GiB of HBM per device.

```python
import jax
import jax.numpy as jnp
from jax import lax

EP = 8
B_DEV = 32
L_MAX = 256
H = 2048
HEADS = 16
KV_LORA = 512
ROPE = 64
NOPE = 128
VHEAD = 128
EXPERTS = 64
TOP = 6
INTER = 1408
SHARED = 2816

B = EP * B_DEV
KVD = KV_LORA + ROPE
QKD = NOPE + ROPE
LEN_LO = (3 * L_MAX) // 4
EPS = 1e-6
ROPE_BASE = 1.0e4


def rms(v):
    v = v.astype(jnp.float32)
    return v * lax.rsqrt(jnp.mean(v * v, axis=-1, keepdims=True) + EPS)


def rope(v, pos):
    half = v.shape[-1] // 2
    inv = ROPE_BASE ** (-2.0 * jnp.arange(half, dtype=jnp.float32) / v.shape[-1])
    ang = pos.astype(jnp.float32)[..., None] * inv
    cs = jnp.cos(ang)
    sn = jnp.sin(ang)
    v1 = v[..., :half]
    v2 = v[..., half:]
    return jnp.concatenate([v1 * cs - v2 * sn, v2 * cs + v1 * sn], axis=-1)


def swiglu(u, wg, wu, wd):
    g = jnp.dot(u, wg, preferred_element_type=jnp.float32)
    v = jnp.dot(u, wu, preferred_element_type=jnp.float32)
    return jnp.dot((jax.nn.silu(g) * v).astype(jnp.bfloat16), wd, preferred_element_type=jnp.float32)


def setup_inputs(seed: int = 0, part: int = 0) -> dict:
    kbase = jax.random.fold_in(jax.random.key(seed), part)
    kp = jax.random.split(kbase, 8)
    kd = jax.random.split(jax.random.fold_in(kbase, 7), 3)
    kw = jax.random.split(jax.random.key(seed + 1), 11)

    def draw(k, shape, fan):
        return (jax.random.normal(k, shape, jnp.float32) * fan ** -0.5).astype(jnp.bfloat16)

    x = jax.random.normal(kp[0], (B, H), jnp.float32).astype(jnp.bfloat16)
    span = (L_MAX - LEN_LO) // 8
    dev = jnp.arange(B) // B_DEV
    low = jax.random.randint(kd[0], (B,), LEN_LO, LEN_LO + span)
    high = jax.random.randint(kd[1], (B,), L_MAX - span, L_MAX)
    lens = jnp.where(dev % 2 == 0, low, high).astype(jnp.int32)
    pos = jnp.arange(L_MAX)[None, :, None]
    m_live = 0.7 * jax.random.normal(kp[2], (B, 1, KVD), jnp.float32)
    m_old = 0.7 * jax.random.normal(kp[3], (B, 1, KVD), jnp.float32)
    noise = jax.random.normal(kp[4], (B, L_MAX, KVD), jnp.float32)
    cache = (jnp.where(pos < lens[:, None, None], m_live, m_old) + noise).astype(jnp.bfloat16)

    def route(k):
        k1, k2 = jax.random.split(k)
        perm_e = jax.random.permutation(k1, EXPERTS)
        perm_t = jax.random.permutation(k2, B_DEV)
        j = jnp.arange(B_DEV)[:, None] * TOP + jnp.arange(TOP)[None, :]
        return perm_e[j % (EXPERTS // 2)][perm_t]

    ids = jax.vmap(route)(jax.random.split(kd[2], EP)).reshape(B, TOP).astype(jnp.int32)
    rw = jax.random.uniform(kp[6], (B, TOP), jnp.float32, 0.5, 1.5) * TOP ** -0.5
    return {
        'x': x,
        'cache': cache,
        'lens': lens,
        'ids': ids,
        'rw': rw,
        'w_q': draw(kw[0], (H, HEADS * QKD), H),
        'w_dkv': draw(kw[1], (H, KVD), H),
        'w_uk': draw(kw[2], (HEADS, NOPE, KV_LORA), NOPE),
        'w_uv': draw(kw[3], (HEADS, KV_LORA, VHEAD), KV_LORA),
        'w_o': draw(kw[4], (HEADS * VHEAD, H), HEADS * VHEAD),
        's_gate': draw(kw[5], (H, SHARED), H),
        's_up': draw(kw[6], (H, SHARED), H),
        's_down': draw(kw[7], (SHARED, H), SHARED),
        'e_gate': draw(kw[8], (EXPERTS, H, INTER), H),
        'e_up': draw(kw[9], (EXPERTS, H, INTER), H),
        'e_down': draw(kw[10], (EXPERTS, INTER, H), INTER),
    }


def reference(x, cache, lens, ids, rw, w_q, w_dkv, w_uk, w_uv, w_o, s_gate, s_up, s_down, e_gate, e_up, e_down):
    xn = rms(x).astype(jnp.bfloat16)
    q = jnp.dot(xn, w_q, preferred_element_type=jnp.float32).astype(jnp.bfloat16).reshape(B, HEADS, QKD)
    kv = jnp.dot(xn, w_dkv, preferred_element_type=jnp.float32)
    kv_new = jnp.concatenate([rms(kv[:, :KV_LORA]), rope(kv[:, KV_LORA:], lens)], axis=-1).astype(jnp.bfloat16)
    q_lat = jnp.einsum('bhd,hdc->bhc', q[:, :, :NOPE].astype(jnp.float32), w_uk.astype(jnp.float32)).astype(jnp.bfloat16)
    q_rot = rope(q[:, :, NOPE:].astype(jnp.float32), lens[:, None]).astype(jnp.bfloat16)
    qf = jnp.concatenate([q_lat, q_rot], axis=-1)
    scale = QKD ** -0.5

    def attend(args):
        qb, cb, kb, lb = args
        qs = qb.astype(jnp.float32)
        cs = cb.astype(jnp.float32)
        ks = kb.astype(jnp.float32)
        s = jnp.dot(qs, cs.T) * scale
        s = jnp.where(jnp.arange(L_MAX)[None, :] < lb, s, -jnp.inf)
        s_new = jnp.dot(qs, ks) * scale
        mx = jnp.maximum(jnp.max(s, axis=1), s_new)
        e = jnp.exp(s - mx[:, None])
        e_new = jnp.exp(s_new - mx)
        den = jnp.sum(e, axis=1) + e_new
        p = (e / den[:, None]).astype(jnp.bfloat16).astype(jnp.float32)
        p_new = (e_new / den).astype(jnp.bfloat16).astype(jnp.float32)
        o = jnp.dot(p, cs[:, :KV_LORA]) + p_new[:, None] * ks[None, :KV_LORA]
        return o.astype(jnp.bfloat16)

    o_lat = lax.map(attend, (qf, cache, kv_new, lens))
    o = jnp.einsum('bhc,hcv->bhv', o_lat.astype(jnp.float32), w_uv.astype(jnp.float32)).astype(jnp.bfloat16).reshape(B, HEADS * VHEAD)
    a = jnp.dot(o, w_o, preferred_element_type=jnp.float32)
    h1 = (x.astype(jnp.float32) + a).astype(jnp.bfloat16)
    u = rms(h1).astype(jnp.bfloat16)
    shared = swiglu(u, s_gate, s_up, s_down)
    gate_w = jnp.sum(jnp.where(ids[:, :, None] == jnp.arange(EXPERTS)[None, None, :], rw[:, :, None], 0.0), axis=1)

    def expert(acc, args):
        wg, wu, wd, cw = args
        out = swiglu(u, wg, wu, wd).astype(jnp.bfloat16).astype(jnp.float32)
        return acc + cw[:, None] * out, None

    routed, _ = lax.scan(expert, jnp.zeros((B, H), jnp.float32), (e_gate, e_up, e_down, gate_w.T))
    y = (h1.astype(jnp.float32) + shared + routed).astype(jnp.bfloat16)
    return y, kv_new
```

```python
import functools

import jax
import jax.numpy as jnp
from jax import lax
from jax.experimental import pallas as pl
from jax.experimental.pallas import tpu as pltpu
from jax.sharding import PartitionSpec as P

EPS = 1e-6
ROPE_BASE = 1.0e4
CAP_FACTOR = 2
N_A = 5
N_B = 3
CW = 256
F32 = jnp.float32
BF16 = jnp.bfloat16


def rms(v):
    v = v.astype(jnp.float32)
    return v * lax.rsqrt(jnp.mean(v * v, axis=-1, keepdims=True) + EPS)


def rope(v, pos):
    half = v.shape[-1] // 2
    inv = ROPE_BASE ** (-2.0 * jnp.arange(half, dtype=jnp.float32) / v.shape[-1])
    ang = pos.astype(jnp.float32)[..., None] * inv
    cs = jnp.cos(ang)
    sn = jnp.sin(ang)
    v1 = v[..., :half]
    v2 = v[..., half:]
    return jnp.concatenate([v1 * cs - v2 * sn, v2 * cs + v1 * sn], axis=-1)


def attention(x, cache, lens, w_q, w_dkv, w_uk, w_uv, w_o):
    bsz = x.shape[0]
    heads, nope, kvl = w_uk.shape
    kvd = cache.shape[2]
    vh = w_uv.shape[2]
    qkd = nope + kvd - kvl
    xn = rms(x).astype(jnp.bfloat16)
    q = jnp.dot(xn, w_q, preferred_element_type=jnp.float32).astype(jnp.bfloat16).reshape(bsz, heads, qkd)
    kv = jnp.dot(xn, w_dkv, preferred_element_type=jnp.float32)
    kv_new = jnp.concatenate([rms(kv[:, :kvl]), rope(kv[:, kvl:], lens)], axis=-1).astype(jnp.bfloat16)
    q_lat = jnp.einsum('bhd,hdc->bhc', q[:, :, :nope], w_uk, preferred_element_type=jnp.float32).astype(jnp.bfloat16)
    q_rot = rope(q[:, :, nope:].astype(jnp.float32), lens[:, None]).astype(jnp.bfloat16)
    qf = jnp.concatenate([q_lat, q_rot], axis=-1)
    scale = qkd ** -0.5
    s = jnp.einsum('bhc,blc->bhl', qf, cache, preferred_element_type=jnp.float32) * scale
    live = jnp.arange(cache.shape[1])[None, None, :] < lens[:, None, None]
    s = jnp.where(live, s, -jnp.inf)
    s_new = jnp.einsum('bhc,bc->bh', qf, kv_new, preferred_element_type=jnp.float32) * scale
    mx = jnp.maximum(jnp.max(s, axis=2), s_new)
    e = jnp.exp(s - mx[:, :, None])
    e_new = jnp.exp(s_new - mx)
    den = jnp.sum(e, axis=2) + e_new
    p = (e / den[:, :, None]).astype(jnp.bfloat16)
    p_new = (e_new / den).astype(jnp.bfloat16)
    o_all = jnp.einsum('bhl,blc->bhc', p, cache, preferred_element_type=jnp.float32)
    o_lat = (o_all[:, :, :kvl] + p_new.astype(jnp.float32)[:, :, None] * kv_new[:, None, :kvl].astype(jnp.float32)).astype(jnp.bfloat16)
    o = jnp.einsum('bhc,hcv->bhv', o_lat, w_uv, preferred_element_type=jnp.float32).astype(jnp.bfloat16).reshape(bsz, heads * vh)
    a = jnp.dot(o, w_o, preferred_element_type=jnp.float32)
    return (x.astype(jnp.float32) + a).astype(jnp.bfloat16), kv_new


def moe_kernel(n, cap, u_ref, h1_ref, meta_ref, eg, eu, ed, sg, su, sd, y_ref,
               wa, wb, meta_all, u_all, xr, act, disp, comb_t, comb, rows,
               pown, psend, precv, zsum, zrecv, sact,
               sem_a, sem_b, ms, mr, us, ur, fs, fr, ps, pr, zs, zr):
    me = lax.axis_index('ep')
    nz = n // 2
    zi = me // 2
    co = lax.rem(me, 2)
    mate = zi * 2 + 1 - co
    b_dev, hid = u_ref.shape
    e_loc, _, inter = eg.shape
    slots = e_loc * cap
    n_tok = n * b_dev
    half = nz * b_dev
    n_ch = hid // CW

    def dev(d):
        return {'ep': d}

    def at_z(dz):
        return lax.rem(zi + dz, nz) * 2 + co

    def from_z(dz):
        return lax.rem(zi + nz - dz, nz)

    def a_copy(src, slot):
        return pltpu.make_async_copy(src, wa.at[slot], sem_a.at[slot])

    def start_gu(e, k):
        a_copy(eg.at[e], lax.rem(2 * e, N_A)).start()
        a_copy(eu.at[e], lax.rem(2 * e + 1, N_A)).start()

    def start_down(j):
        slot = lax.rem(j, N_B)
        for e in range(e_loc):
            pltpu.make_async_copy(
                ed.at[e, :, pl.ds(pl.multiple_of(j * CW, CW), CW)],
                wb.at[slot, :, pl.ds(e * CW, CW)], sem_b.at[slot]).start()

    def wait_a(slot):
        a_copy(eg.at[0], slot).wait()

    def wait_b(slot):
        pltpu.make_async_copy(sd.at[pl.ds(0, inter)], wb.at[slot], sem_b.at[slot]).wait()

    n_gu = 2 * e_loc
    sh_a = [(sg, 0), (su, 0), (sg, 1), (su, 1)]

    def start_unit_a(i):
        slot = i % N_A
        if i < n_gu:
            a_copy((eg if i % 2 == 0 else eu).at[i // 2], slot).start()
        else:
            r, h = sh_a[i - n_gu]
            a_copy(r.at[:, pl.ds(h * inter, inter)], slot).start()

    for i in range(N_A):
        start_unit_a(i)
    for j in range(N_B):
        start_down(j)

    barrier = pltpu.get_barrier_semaphore()
    for d in range(1, n):
        pl.semaphore_signal(barrier, inc=1, device_id=dev(lax.rem(me + d, n)))
    pl.semaphore_wait(barrier, n - 1)

    def meta_copy(d):
        return pltpu.make_async_remote_copy(
            meta_ref, meta_all.at[me], ms.at[d - 1], mr.at[d - 1],
            device_id=dev(lax.rem(me + d, n)), device_id_type=pl.DeviceIdType.MESH)

    my_rows = pl.ds(pl.multiple_of(me * b_dev, b_dev), b_dev)

    def u_copy(k, target):
        return pltpu.make_async_remote_copy(
            u_ref, u_all.at[my_rows], us.at[k], ur.at[k],
            device_id=dev(target), device_id_type=pl.DeviceIdType.MESH)

    def fwd_copy(dz):
        blk = from_z(dz) * 2 + co
        r = u_all.at[pl.ds(pl.multiple_of(blk * b_dev, b_dev), b_dev)]
        return pltpu.make_async_remote_copy(
            r, r, fs.at[dz - 1], fr.at[dz - 1],
            device_id=dev(mate), device_id_type=pl.DeviceIdType.MESH)

    def recv_wait(dst, sem):
        pltpu.make_async_remote_copy(
            dst, dst, us.at[0], sem, device_id=dev(mate),
            device_id_type=pl.DeviceIdType.MESH).wait_recv()

    for d in range(1, n):
        meta_copy(d).start()
    for dz in range(1, nz):
        u_copy(dz - 1, at_z(dz)).start()
    u_copy(nz - 1, mate).start()
    u_all[my_rows] = u_ref[...]

    tot = meta_ref[...]
    for d in range(1, n):
        src = lax.rem(me + n - d, n)
        recv_wait(meta_all.at[src], mr.at[d - 1])
        tot = tot + meta_all[src]
    half_m = tot.shape[0] // 2
    lane = lax.broadcasted_iota(jnp.int32, (e_loc, n_tok), 0) + (me * e_loc + 1)
    lane = lane.astype(F32)
    hit = jnp.zeros((e_loc, n_tok), F32)
    wt = jnp.zeros((e_loc, n_tok), F32)
    for k in range(half_m):
        eq = tot[k:k + 1] == lane
        hit = hit + jnp.where(eq, 1.0, 0.0)
        wt = wt + jnp.where(eq, tot[half_m + k:half_m + k + 1], 0.0)
    r0 = lax.broadcasted_iota(jnp.int32, (n_tok, n_tok), 0)
    r1 = lax.broadcasted_iota(jnp.int32, (n_tok, n_tok), 1)
    before = jnp.where(r0 < r1, 1.0, 0.0).astype(BF16)
    rank = jnp.dot(hit.astype(BF16), before, preferred_element_type=F32)
    rank = jnp.where(hit > 0.5, rank, -1.0)
    w1 = wt.astype(BF16).astype(F32)
    rest = wt - w1
    w2 = rest.astype(BF16).astype(F32)
    w3 = rest - w2
    row = lax.broadcasted_iota(jnp.int32, (cap, n_tok), 0).astype(F32)
    for e in range(e_loc):
        m = row == rank[e:e + 1]
        disp[e * cap:(e + 1) * cap] = jnp.where(m, 1.0, 0.0).astype(BF16)
        for p, w in enumerate((w1, w2, w3)):
            comb_t[p * slots + e * cap:p * slots + (e + 1) * cap] = jnp.where(m, w[e:e + 1], 0.0).astype(BF16)
    side = r0 // half
    blk = lax.rem(r0, half) // b_dev
    chip = lax.rem(blk + zi, nz)
    core = jnp.where(side == 0, co, 1 - co)
    tok = (chip * 2 + core) * b_dev + lax.rem(r0, b_dev)
    perm = jnp.where(r1 == tok, 1.0, 0.0).astype(BF16)
    comb[...] = lax.dot_general(perm, comb_t[...], (((1,), (1,)), ((), ())),
                                preferred_element_type=F32).astype(BF16)

    for dz in range(1, nz):
        blk_z = from_z(dz) * 2 + co
        recv_wait(u_all.at[pl.ds(pl.multiple_of(blk_z * b_dev, b_dev), b_dev)], ur.at[dz - 1])
        fwd_copy(dz).start()
    recv_wait(u_all.at[pl.ds(pl.multiple_of(mate * b_dev, b_dev), b_dev)], ur.at[nz - 1])
    for dz in range(1, nz):
        blk_z = from_z(dz) * 2 + 1 - co
        recv_wait(u_all.at[pl.ds(pl.multiple_of(blk_z * b_dev, b_dev), b_dev)], fr.at[dz - 1])

    @pl.loop(0, hid // 512)
    def _(i):
        cols = pl.ds(pl.multiple_of(i * 512, 512), 512)
        xr[:, cols] = jnp.dot(disp[...], u_all[:, cols], preferred_element_type=F32).astype(BF16)

    def gate_up(x, sa, sb, store):
        for c0 in range(0, inter, CW):
            c1 = min(c0 + CW, inter)
            g = jnp.dot(x, wa[sa, :, c0:c1], preferred_element_type=F32)
            v = jnp.dot(x, wa[sb, :, c0:c1], preferred_element_type=F32)
            store(c0, c1, (jax.nn.silu(g) * v).astype(BF16))

    def expert_body(e):
        sa = lax.rem(2 * e, N_A)
        sb = lax.rem(2 * e + 1, N_A)
        wait_a(sa)
        wait_a(sb)
        rs = pl.ds(pl.multiple_of(e * cap, cap), cap)

        def store(c0, c1, val):
            act[rs, c0:c1] = val

        gate_up(xr[rs, :], sa, sb, store)

    @pl.loop(0, e_loc)
    def _(e):
        expert_body(e)
        for t in range(2):
            i = 2 * e + t + N_A
            slot = lax.rem(i, N_A)

            @pl.when(jnp.logical_and(i < n_gu, lax.rem(i, 2) == 0))
            def _():
                a_copy(eg.at[lax.min(i // 2, e_loc - 1)], slot).start()

            @pl.when(jnp.logical_and(i < n_gu, lax.rem(i, 2) == 1))
            def _():
                a_copy(eu.at[lax.min(i // 2, e_loc - 1)], slot).start()

            for q in range(4):
                @pl.when(i == n_gu + q)
                def _():
                    r, h = sh_a[q]
                    a_copy(r.at[:, pl.ds(h * inter, inter)], slot).start()

    def p_copy(j):
        return pltpu.make_async_remote_copy(
            psend.at[j], precv.at[j], ps.at[j], pr.at[j],
            device_id=dev(mate), device_id_type=pl.DeviceIdType.MESH)

    def z_copy(j, dz):
        return pltpu.make_async_remote_copy(
            zsum.at[j, pl.ds(dz * b_dev, b_dev)], zrecv.at[j, dz - 1],
            zs.at[j, dz - 1], zr.at[j, dz - 1],
            device_id=dev(at_z(dz)), device_id_type=pl.DeviceIdType.MESH)

    def pass_on(j):
        recv_wait(precv.at[j], pr.at[j])
        zsum[j] = pown[j] + precv[j]
        for dz in range(1, nz):
            z_copy(j, dz).start()

    @pl.loop(0, n_ch)
    def _(j):
        slot = lax.rem(j, N_B)
        wait_b(slot)
        for e in range(e_loc):
            rows[e * cap:(e + 1) * cap] = jnp.dot(
                act[e * cap:(e + 1) * cap], wb[slot, :, e * CW:(e + 1) * CW],
                preferred_element_type=F32).astype(BF16)

        @pl.when(j + N_B < n_ch)
        def _():
            start_down(lax.min(j + N_B, n_ch - 1))

        for h in range(2):
            i = n_ch + h

            @pl.when(j + N_B == i)
            def _():
                pltpu.make_async_copy(sd.at[pl.ds(h * inter, inter)], wb.at[i % N_B], sem_b.at[i % N_B]).start()

        part = jnp.dot(comb[:, 0:slots], rows[...], preferred_element_type=F32)
        part += jnp.dot(comb[:, slots:2 * slots], rows[...], preferred_element_type=F32)
        part += jnp.dot(comb[:, 2 * slots:3 * slots], rows[...], preferred_element_type=F32)
        pown[j] = part[:half]
        psend[j] = part[half:]
        p_copy(j).start()

        @pl.when(j > 0)
        def _():
            pass_on(lax.max(j - 1, 0))

    for h in range(2):
        sa = (n_gu + 2 * h) % N_A
        sb = (n_gu + 2 * h + 1) % N_A
        wait_a(sa)
        wait_a(sb)

        def store(c0, c1, val):
            sact[:, h * inter + c0:h * inter + c1] = val

        gate_up(u_ref[...], sa, sb, store)
        if h == 0:
            pass_on(n_ch - 1)
    for h in range(2):
        wait_b((n_ch + h) % N_B)

    for j in range(n_ch):
        cols = slice(j * CW, (j + 1) * CW)
        s = jnp.dot(sact[:, :inter], wb[n_ch % N_B, :, cols], preferred_element_type=F32)
        s += jnp.dot(sact[:, inter:], wb[(n_ch + 1) % N_B, :, cols], preferred_element_type=F32)
        routed = zsum[j, :b_dev]
        for dz in range(1, nz):
            recv_wait(zrecv.at[j, dz - 1], zr.at[j, dz - 1])
            routed = routed + zrecv[j, dz - 1]
        y_ref[:, cols] = (h1_ref[:, cols].astype(F32) + s + routed).astype(BF16)

    for d in range(1, n):
        meta_copy(d).wait_send()
    for dz in range(1, nz):
        u_copy(dz - 1, at_z(dz)).wait_send()
        fwd_copy(dz).wait_send()
    u_copy(nz - 1, mate).wait_send()
    for j in range(n_ch):
        p_copy(j).wait_send()
        for dz in range(1, nz):
            z_copy(j, dz).wait_send()


def moe(n, u, h1, meta, eg, eu, ed, sg, su, sd, cap):
    b_dev, hid = u.shape
    e_loc, _, inter = eg.shape
    n_tok = n * b_dev
    slots = e_loc * cap
    nz = n // 2
    half = nz * b_dev
    n_ch = hid // CW
    dma = pltpu.SemaphoreType.DMA
    vm = pl.BlockSpec(memory_space=pltpu.VMEM)
    anys = pl.BlockSpec(memory_space=pl.ANY)
    flops = 2 * 3 * hid * inter * (slots + 2 * b_dev)
    return pl.pallas_call(
        functools.partial(moe_kernel, n, cap),
        out_shape=jax.ShapeDtypeStruct((b_dev, hid), BF16),
        in_specs=[vm, vm, vm] + [anys] * 6,
        out_specs=vm,
        scratch_shapes=[
            pltpu.VMEM((N_A, hid, inter), BF16),
            pltpu.VMEM((N_B, inter, hid), BF16),
            pltpu.VMEM((n,) + meta.shape, F32),
            pltpu.VMEM((n_tok, hid), BF16),
            pltpu.VMEM((slots, hid), BF16),
            pltpu.VMEM((slots, inter), BF16),
            pltpu.VMEM((slots, n_tok), BF16),
            pltpu.VMEM((3 * slots, n_tok), BF16),
            pltpu.VMEM((n_tok, 3 * slots), BF16),
            pltpu.VMEM((slots, CW), BF16),
            pltpu.VMEM((n_ch, half, CW), F32),
            pltpu.VMEM((n_ch, half, CW), F32),
            pltpu.VMEM((n_ch, half, CW), F32),
            pltpu.VMEM((n_ch, half, CW), F32),
            pltpu.VMEM((n_ch, nz - 1, b_dev, CW), F32),
            pltpu.VMEM((b_dev, 2 * inter), BF16),
            dma((N_A,)), dma((N_B,)),
            dma((n - 1,)), dma((n - 1,)),
            dma((nz,)), dma((nz,)),
            dma((nz - 1,)), dma((nz - 1,)),
            dma((n_ch,)), dma((n_ch,)),
            dma((n_ch, nz - 1)), dma((n_ch, nz - 1)),
        ],
        compiler_params=pltpu.CompilerParams(
            collective_id=0, has_side_effects=True, vmem_limit_bytes=63 << 20),
        cost_estimate=pl.CostEstimate(flops=flops, bytes_accessed=30 * hid * inter * 2, transcendentals=0),
        name="moe",
    )(u, h1, meta, eg, eu, ed, sg, su, sd)


def solution(mesh):
    n = mesh.shape['ep']
    tok_spec = P(('rep', 'ep'))
    row_spec = P(('rep', 'ep'), None)
    cache_spec = P(('rep', 'ep'), None, None)
    exp_spec = P('ep', None, None)

    def local(x, cache, lens, ids, rw, w_q, w_dkv, w_uk, w_uv, w_o, s_gate, s_up, s_down, e_gate, e_up, e_down):
        b_dev, top = ids.shape
        e_loc = e_gate.shape[0]
        n_exp = e_loc * n
        cape = (CAP_FACTOR * b_dev * top + n_exp - 1) // n_exp
        me = lax.axis_index('ep')
        here = (jnp.arange(n * b_dev) // b_dev == me)[None]
        pad = ((0, 8 - top), (0, 0))

        def spread(v):
            return jnp.where(here, jnp.tile(jnp.pad(v.T, pad), (1, n)), 0.0)

        meta = jnp.concatenate([spread(ids.astype(F32) + 1.0), spread(rw.astype(F32))], axis=0)
        h1, kv_new = attention(x, cache, lens, w_q, w_dkv, w_uk, w_uv, w_o)
        u = rms(h1).astype(jnp.bfloat16)
        y = moe(n, u, h1, meta, e_gate, e_up, e_down, s_gate, s_up, s_down, n * cape)
        return y, kv_new

    in_specs = (row_spec, cache_spec, tok_spec, row_spec, row_spec) + (P(),) * 8 + (exp_spec,) * 3
    return jax.shard_map(local, mesh=mesh, in_specs=in_specs, out_specs=(row_spec, row_spec), check_vma=False)
```

```python
import functools
import math

import jax
import jax.numpy as jnp
from jax import lax
from jax.experimental import pallas as pl
from jax.experimental.pallas import tpu as pltpu
from jax.sharding import PartitionSpec as P

EPS = 1e-6
ROPE_BASE = 1.0e4
CAP_FACTOR = 2
N_A = 6
N_B = 2
CW = 256
F32 = jnp.float32
BF16 = jnp.bfloat16


def attn_kernel(x_ref, lrow_ref, lens_ref, ids_ref, rw_ref, wq, wdkv, wuk, wuv, wo, cache,
                h1_ref, u_ref, kvn_ref, meta_ref,
                wq_b, wdkv_b, wuk_b, wuv_b, wo_b, cache_b, q_s, ql_s, qr_s, kv_s, s_s, p_s, ol_s, o_s, sems):
    bsz, hid = x_ref.shape
    heads, nope, kvl = wuk.shape
    kvd = wdkv.shape[0]
    rot = kvd - kvl
    l_max = cache.shape[2]
    qkd = nope + rot
    n_q = 3
    qc = wq.shape[1] // n_q
    n_c = 4
    bc = bsz // n_c
    n_o = 2
    oc = hid // n_o
    copies = []

    def start(src, dst):
        c = pltpu.make_async_copy(src, dst, sems.at[len(copies)])
        c.start()
        copies.append(c)
        return c

    c_q = [start(wq.at[:, i * qc:(i + 1) * qc], wq_b.at[:, i * qc:(i + 1) * qc]) for i in range(n_q)]
    c_kv = start(wdkv, wdkv_b)
    c_uk = start(wuk, wuk_b)
    c_c = [start(cache.at[i * bc:(i + 1) * bc], cache_b.at[i * bc:(i + 1) * bc]) for i in range(n_c)]
    c_uv = start(wuv, wuv_b)
    c_o = [start(wo.at[:, i * oc:(i + 1) * oc], wo_b.at[:, i * oc:(i + 1) * oc]) for i in range(n_o)]

    me = lax.axis_index('ep')
    n_tok = meta_ref.shape[1]
    top = ids_ref.shape[0]
    lane = lax.broadcasted_iota(jnp.int32, (top, n_tok), 1) // bsz
    meta_ref[...] = jnp.zeros_like(meta_ref)
    for r, v in enumerate((ids_ref[...].astype(F32) + 1.0, rw_ref[...])):
        v = jnp.concatenate([v] * (n_tok // bsz), axis=1)
        meta_ref[r * 8:r * 8 + top] = jnp.where(lane == me, v, 0.0)

    eye = lax.broadcasted_iota(jnp.int32, (bsz, bsz), 0) == lax.broadcasted_iota(jnp.int32, (bsz, bsz), 1)
    pos = jnp.sum(jnp.where(eye, lrow_ref[...].astype(F32), 0.0), axis=1, keepdims=True)
    half = rot // 2
    li = lax.broadcasted_iota(jnp.int32, (bsz, rot), 1)
    fi = jnp.where(li < half, li, li - half).astype(F32)
    ang = pos * jnp.exp(fi * (-2.0 / rot * math.log(ROPE_BASE)))
    cs = jnp.cos(ang)
    sn = jnp.sin(ang)
    sn = jnp.where(li < half, -sn, sn)

    def rope(v):
        return v * cs + jnp.concatenate([v[:, half:], v[:, :half]], axis=1) * sn

    def norm(v):
        return v * lax.rsqrt(jnp.mean(v * v, axis=-1, keepdims=True) + EPS)

    xn = norm(x_ref[...].astype(F32)).astype(BF16)
    for i in range(n_q):
        c_q[i].wait()
        q_s[:, i * qc:(i + 1) * qc] = jnp.dot(
            xn, wq_b[:, i * qc:(i + 1) * qc], preferred_element_type=F32).astype(BF16)
    c_kv.wait()
    kv = lax.dot_general(xn, wdkv_b[...], (((1,), (1,)), ((), ())), preferred_element_type=F32)
    kvn_ref[:, :kvl] = norm(kv[:, :kvl]).astype(BF16)
    kvn_ref[:, kvl:] = rope(kv[:, kvl:]).astype(BF16)
    kv_s[:, :kvd] = kvn_ref[...].astype(F32)
    c_uk.wait()
    for h in range(heads):
        c0 = h * qkd
        rs = slice(h * bsz, (h + 1) * bsz)
        ql = jnp.dot(q_s[:, c0:c0 + nope], wuk_b[h], preferred_element_type=F32).astype(BF16).astype(F32)
        for g in range(kvl // 128):
            ql_s[g, rs] = ql[:, g * 128:(g + 1) * 128]
        qr_s[rs, :rot] = rope(q_s[:, c0 + nope:c0 + qkd].astype(F32)).astype(BF16).astype(F32)

    col = lax.broadcasted_iota(jnp.int32, (heads, l_max), 1)
    scale = qkd ** -0.5
    unroll = 8
    for i in range(n_c):
        c_c[i].wait()

        @pl.loop(0, bc // unroll)
        def _(t):
            for k in range(unroll):
                b = i * bc + t * unroll + k
                ql = jnp.concatenate(
                    [ql_s[g, pl.ds(b, heads, stride=bsz), :] for g in range(kvl // 128)], axis=1)
                qr = qr_s[pl.ds(b, heads, stride=bsz), :][:, :rot]
                kl = kv_s[pl.ds(b, 1), :]
                s = jnp.dot(ql.astype(BF16), cache_b[b, :kvl], preferred_element_type=F32)
                s += jnp.dot(qr.astype(BF16), cache_b[b, kvl:], preferred_element_type=F32)
                s_new = jnp.sum(ql * kl[:, :kvl], axis=1, keepdims=True)
                s_new += jnp.sum(qr * kl[:, kvl:kvd], axis=1, keepdims=True)
                n_live = lens_ref[b]
                s = jnp.where(col < n_live, s, jnp.where(col == n_live, s_new, -jnp.inf)) * scale
                s_s[pl.ds(pl.multiple_of(b * heads, heads), heads)] = s

    blk = 128

    @pl.loop(0, bsz * heads // blk)
    def _(t):
        rs = pl.ds(pl.multiple_of(t * blk, blk), blk)
        s = s_s[rs]
        e = jnp.exp(s - jnp.max(s, axis=1, keepdims=True))
        p_s[rs] = (e / jnp.sum(e, axis=1, keepdims=True)).astype(BF16)

    @pl.loop(0, bsz // unroll)
    def _(t):
        for k in range(unroll):
            b = t * unroll + k
            rs = pl.ds(pl.multiple_of(b * heads, heads), heads)
            n_live = lens_ref[b]
            p = p_s[rs].astype(F32)
            p_old = jnp.where(col < n_live, p, 0.0).astype(BF16)
            p_new = jnp.sum(jnp.where(col == n_live, p, 0.0), axis=1, keepdims=True)
            o = lax.dot_general(p_old, cache_b[b, :kvl], (((1,), (1,)), ((), ())), preferred_element_type=F32)
            o += p_new * kv_s[pl.ds(b, 1), :][:, :kvl]
            o = o.astype(BF16).astype(F32)
            for g in range(kvl // 128):
                ol_s[g, rs] = o[:, g * 128:(g + 1) * 128]

    c_uv.wait()
    vh = wuv.shape[2]
    for h in range(heads):
        oh = jnp.concatenate(
            [ol_s[g, pl.ds(h, bsz, stride=heads), :] for g in range(kvl // 128)], axis=1).astype(BF16)
        o_s[:, h * vh:(h + 1) * vh] = jnp.dot(oh, wuv_b[h], preferred_element_type=F32).astype(BF16)
    sq = jnp.zeros((bsz, 1), F32)
    for i in range(n_o):
        c_o[i].wait()
        cols = slice(i * oc, (i + 1) * oc)
        a = jnp.dot(o_s[...], wo_b[:, cols], preferred_element_type=F32)
        h1 = (x_ref[:, cols].astype(F32) + a).astype(BF16)
        h1_ref[:, cols] = h1
        h1 = h1.astype(F32)
        sq += jnp.sum(h1 * h1, axis=1, keepdims=True)
    u_ref[...] = (h1_ref[...].astype(F32) * lax.rsqrt(sq / hid + EPS)).astype(BF16)


def attention(n, x, cache, lens, ids, rw, w_q, w_dkv, w_uk, w_uv, w_o):
    bsz, hid = x.shape
    heads, nope, kvl = w_uk.shape
    l_max, kvd = cache.shape[1:]
    vm = pl.BlockSpec(memory_space=pltpu.VMEM)
    anys = pl.BlockSpec(memory_space=pl.ANY)
    cache_t = jnp.swapaxes(cache, 1, 2)
    rows = bsz * heads
    weights = (w_q, w_dkv.T, w_uk, w_uv, w_o, cache_t)
    row = jax.ShapeDtypeStruct((bsz, hid), BF16)
    return pl.pallas_call(
        attn_kernel,
        out_shape=(row, row, jax.ShapeDtypeStruct((bsz, kvd), BF16), jax.ShapeDtypeStruct((16, n * bsz), F32)),
        in_specs=[vm, vm, pl.BlockSpec(memory_space=pltpu.SMEM), vm, vm] + [anys] * 6,
        out_specs=(vm,) * 4,
        scratch_shapes=[pltpu.VMEM(w.shape, BF16) for w in weights] + [
            pltpu.VMEM((bsz, w_q.shape[1]), BF16),
            pltpu.VMEM((kvl // 128, rows, 128), F32),
            pltpu.VMEM((rows, 128), F32),
            pltpu.VMEM((bsz, kvl + 128), F32),
            pltpu.VMEM((rows, l_max), F32),
            pltpu.VMEM((rows, l_max), BF16),
            pltpu.VMEM((kvl // 128, rows, 128), F32),
            pltpu.VMEM((bsz, w_o.shape[0]), BF16),
            pltpu.SemaphoreType.DMA((12,)),
        ],
        compiler_params=pltpu.CompilerParams(vmem_limit_bytes=60 << 20),
        cost_estimate=pl.CostEstimate(
            flops=2 * bsz * (hid * (w_q.shape[1] + kvd + w_o.shape[0]) + heads * kvl * (2 * nope + 2 * l_max)),
            bytes_accessed=2 * sum(w.size for w in weights), transcendentals=rows * l_max),
        name="attn",
    )(x, lens.reshape(1, bsz), lens, ids.T, rw.T, *weights)


def moe_kernel(n, cap, u_ref, h1_ref, meta_ref, eg, eu, ed, sg, su, sd, y_ref,
               wa, wb, meta_all, u_all, xr, act, disp, comb_t, comb, rows,
               pown, psend, precv, zsum, zside, zrecv, sact,
               sem_a, sem_b, ms, mr, us, ur, fs, fr, ps, pr, zs, zr):
    me = lax.axis_index('ep')
    nz = n // 2
    zi = me // 2
    co = lax.rem(me, 2)
    mate = zi * 2 + 1 - co
    b_dev, hid = u_ref.shape
    e_loc, _, inter = eg.shape
    slots = e_loc * cap
    n_tok = n * b_dev
    half = nz * b_dev
    n_ch = hid // CW

    def dev(d):
        return {'ep': d}

    low = zi < 2
    inner = jnp.logical_or(zi == 1, zi == 2)
    beside = jnp.where(low, 1 - zi, 5 - zi)
    across = jnp.where(low, 2, 1)
    far = jnp.where(low, 3, 0)
    others = (far, across, beside)

    def on(z):
        return dev(z * 2 + co)

    def a_copy(src, slot):
        return pltpu.make_async_copy(src, wa.at[slot], sem_a.at[slot])

    def start_gu(e, k):
        a_copy(eg.at[e], lax.rem(2 * e, N_A)).start()
        a_copy(eu.at[e], lax.rem(2 * e + 1, N_A)).start()

    def start_down(j):
        slot = lax.rem(j, N_B)
        for e in range(e_loc):
            pltpu.make_async_copy(
                ed.at[e, :, pl.ds(pl.multiple_of(j * CW, CW), CW)],
                wb.at[slot, :, pl.ds(e * CW, CW)], sem_b.at[slot]).start()

    def wait_a(slot):
        a_copy(eg.at[0], slot).wait()

    def wait_b(slot):
        pltpu.make_async_copy(sd.at[pl.ds(0, inter)], wb.at[slot], sem_b.at[slot]).wait()

    n_gu = 2 * e_loc
    sh_a = [(sg, 0), (su, 0), (sg, 1), (su, 1)]

    def start_unit_a(i):
        slot = i % N_A
        if i < n_gu:
            a_copy((eg if i % 2 == 0 else eu).at[i // 2], slot).start()
        else:
            r, h = sh_a[i - n_gu]
            a_copy(r.at[:, pl.ds(h * inter, inter)], slot).start()

    for i in range(N_A):
        start_unit_a(i)
    for j in range(N_B):
        start_down(j)

    barrier = pltpu.get_barrier_semaphore()
    for d in range(1, n):
        pl.semaphore_signal(barrier, inc=1, device_id=dev(lax.rem(me + d, n)))
    pl.semaphore_wait(barrier, n - 1)

    def meta_copy(d):
        return pltpu.make_async_remote_copy(
            meta_ref, meta_all.at[me], ms.at[d - 1], mr.at[d - 1],
            device_id=dev(lax.rem(me + d, n)), device_id_type=pl.DeviceIdType.MESH)

    my_rows = pl.ds(pl.multiple_of(me * b_dev, b_dev), b_dev)

    def u_copy(k, target):
        return pltpu.make_async_remote_copy(
            u_ref, u_all.at[my_rows], us.at[k], ur.at[zi if k < nz - 1 else nz],
            device_id=target, device_id_type=pl.DeviceIdType.MESH)

    def u_rows(z, c):
        return u_all.at[pl.ds(pl.multiple_of((z * 2 + c) * b_dev, b_dev), b_dev)]

    def fwd_copy(z):
        r = u_rows(z, co)
        return pltpu.make_async_remote_copy(
            r, r, fs.at[z], fr.at[z],
            device_id=dev(mate), device_id_type=pl.DeviceIdType.MESH)

    def recv_wait(dst, sem):
        pltpu.make_async_remote_copy(
            dst, dst, us.at[0], sem, device_id=dev(mate),
            device_id_type=pl.DeviceIdType.MESH).wait_recv()

    for d in range(1, n):
        meta_copy(d).start()
    for k, z in enumerate(others):
        u_copy(k, on(z)).start()
    u_copy(nz - 1, dev(mate)).start()
    u_all[my_rows] = u_ref[...]

    tot = meta_ref[...]
    for d in range(1, n):
        src = lax.rem(me + n - d, n)
        recv_wait(meta_all.at[src], mr.at[d - 1])
        tot = tot + meta_all[src]
    half_m = tot.shape[0] // 2
    lane = lax.broadcasted_iota(jnp.int32, (e_loc, n_tok), 0) + (me * e_loc + 1)
    lane = lane.astype(F32)
    hit = jnp.zeros((e_loc, n_tok), F32)
    wt = jnp.zeros((e_loc, n_tok), F32)
    for k in range(half_m):
        eq = tot[k:k + 1] == lane
        hit = hit + jnp.where(eq, 1.0, 0.0)
        wt = wt + jnp.where(eq, tot[half_m + k:half_m + k + 1], 0.0)
    r0 = lax.broadcasted_iota(jnp.int32, (n_tok, n_tok), 0)
    r1 = lax.broadcasted_iota(jnp.int32, (n_tok, n_tok), 1)
    before = jnp.where(r0 < r1, 1.0, 0.0).astype(BF16)
    rank = jnp.dot(hit.astype(BF16), before, preferred_element_type=F32)
    rank = jnp.where(hit > 0.5, rank, -1.0)
    w1 = wt.astype(BF16).astype(F32)
    rest = wt - w1
    w2 = rest.astype(BF16).astype(F32)
    w3 = rest - w2
    row = lax.broadcasted_iota(jnp.int32, (cap, n_tok), 0).astype(F32)
    for e in range(e_loc):
        m = row == rank[e:e + 1]
        disp[e * cap:(e + 1) * cap] = jnp.where(m, 1.0, 0.0).astype(BF16)
        for p, w in enumerate((w1, w2, w3)):
            comb_t[p * slots + e * cap:p * slots + (e + 1) * cap] = jnp.where(m, w[e:e + 1], 0.0).astype(BF16)
    side = r0 // half
    blk = lax.rem(r0, half) // b_dev
    chip = jnp.where(blk == 0, zi, jnp.where(blk == 1, beside, jnp.where(blk == 2, across, far)))
    core = jnp.where(side == 0, co, 1 - co)
    tok = (chip * 2 + core) * b_dev + lax.rem(r0, b_dev)
    perm = jnp.where(r1 == tok, 1.0, 0.0).astype(BF16)
    comb[...] = lax.dot_general(perm, comb_t[...], (((1,), (1,)), ((), ())),
                                preferred_element_type=F32).astype(BF16)

    recv_wait(u_rows(zi, 1 - co), ur.at[nz])
    for z in (beside, across, far):
        recv_wait(u_rows(z, co), ur.at[z])
        fwd_copy(z).start()
    for z in (beside, across, far):
        recv_wait(u_rows(z, 1 - co), fr.at[z])

    @pl.loop(0, hid // 512)
    def _(i):
        cols = pl.ds(pl.multiple_of(i * 512, 512), 512)
        xr[:, cols] = jnp.dot(disp[...], u_all[:, cols], preferred_element_type=F32).astype(BF16)

    def gate_up(x, sa, sb, store):
        for c0 in range(0, inter, CW):
            c1 = min(c0 + CW, inter)
            g = jnp.dot(x, wa[sa, :, c0:c1], preferred_element_type=F32)
            v = jnp.dot(x, wa[sb, :, c0:c1], preferred_element_type=F32)
            store(c0, c1, (jax.nn.silu(g) * v).astype(BF16))

    def expert_body(e):
        sa = lax.rem(2 * e, N_A)
        sb = lax.rem(2 * e + 1, N_A)
        wait_a(sa)
        wait_a(sb)
        rs = pl.ds(pl.multiple_of(e * cap, cap), cap)

        def store(c0, c1, val):
            act[rs, c0:c1] = val

        gate_up(xr[rs, :], sa, sb, store)

    @pl.loop(0, e_loc)
    def _(e):
        expert_body(e)
        for t in range(2):
            i = 2 * e + t + N_A
            slot = lax.rem(i, N_A)

            @pl.when(jnp.logical_and(i < n_gu, lax.rem(i, 2) == 0))
            def _():
                a_copy(eg.at[lax.min(i // 2, e_loc - 1)], slot).start()

            @pl.when(jnp.logical_and(i < n_gu, lax.rem(i, 2) == 1))
            def _():
                a_copy(eu.at[lax.min(i // 2, e_loc - 1)], slot).start()

            for q in range(4):
                @pl.when(i == n_gu + q)
                def _():
                    r, h = sh_a[q]
                    a_copy(r.at[:, pl.ds(h * inter, inter)], slot).start()

    def p_copy(j):
        return pltpu.make_async_remote_copy(
            psend.at[j], precv.at[j], ps.at[j], pr.at[j],
            device_id=dev(mate), device_id_type=pl.DeviceIdType.MESH)

    def to_beside(j, size):
        return pltpu.make_async_remote_copy(
            zsum.at[j, pl.ds(b_dev, size * b_dev)], zside.at[j, pl.ds(0, size * b_dev)],
            zs.at[j, 0], zr.at[j, 0], device_id=on(beside), device_id_type=pl.DeviceIdType.MESH)

    def to_other(j, k, z):
        return pltpu.make_async_remote_copy(
            zsum.at[j, pl.ds((2 + k) * b_dev, b_dev)], zrecv.at[j],
            zs.at[j, 1 + k], zr.at[j, 1], device_id=on(z), device_id_type=pl.DeviceIdType.MESH)

    def chip_sum(j):
        recv_wait(precv.at[j], pr.at[j])
        zsum[j] = pown[j] + precv[j]

        @pl.when(inner)
        def _():
            to_beside(j, 1).start()

        @pl.when(jnp.logical_not(inner))
        def _():
            to_beside(j, nz - 1).start()

    def wait_beside(j):
        @pl.when(jnp.logical_not(inner))
        def _():
            recv_wait(zside.at[j, pl.ds(0, b_dev)], zr.at[j, 0])

    def relay(j):
        @pl.when(inner)
        def _():
            recv_wait(zside.at[j], zr.at[j, 0])
            zsum[j, 2 * b_dev:] = zsum[j, 2 * b_dev:] + zside[j, b_dev:]
            to_other(j, 1, far).start()
            to_other(j, 0, across).start()

    @pl.loop(0, n_ch)
    def _(j):
        slot = lax.rem(j, N_B)
        wait_b(slot)
        for e in range(e_loc):
            rows[e * cap:(e + 1) * cap] = jnp.dot(
                act[e * cap:(e + 1) * cap], wb[slot, :, e * CW:(e + 1) * CW],
                preferred_element_type=F32).astype(BF16)

        @pl.when(j + N_B < n_ch)
        def _():
            start_down(lax.min(j + N_B, n_ch - 1))

        for h in range(2):
            i = n_ch + h

            @pl.when(j + N_B == i)
            def _():
                pltpu.make_async_copy(sd.at[pl.ds(h * inter, inter)], wb.at[i % N_B], sem_b.at[i % N_B]).start()

        part = jnp.dot(comb[:, 0:slots], rows[...], preferred_element_type=F32)
        part += jnp.dot(comb[:, slots:2 * slots], rows[...], preferred_element_type=F32)
        part += jnp.dot(comb[:, 2 * slots:3 * slots], rows[...], preferred_element_type=F32)
        pown[j] = part[:half]
        psend[j] = part[half:]
        p_copy(j).start()

        @pl.when(j > 0)
        def _():
            chip_sum(lax.max(j - 1, 0))

        @pl.when(j > 1)
        def _():
            relay(lax.max(j - 2, 0))

    for h in range(2):
        sa = (n_gu + 2 * h) % N_A
        sb = (n_gu + 2 * h + 1) % N_A
        wait_a(sa)
        wait_a(sb)

        def store(c0, c1, val):
            sact[:, h * inter + c0:h * inter + c1] = val

        gate_up(u_ref[...], sa, sb, store)
        if h == 0:
            chip_sum(n_ch - 1)
            relay(n_ch - 2)
        else:
            relay(n_ch - 1)
    for h in range(2):
        wait_b((n_ch + h) % N_B)

    for j in range(n_ch):
        cols = slice(j * CW, (j + 1) * CW)
        s = jnp.dot(sact[:, :inter], wb[n_ch % N_B, :, cols], preferred_element_type=F32)
        s += jnp.dot(sact[:, inter:], wb[(n_ch + 1) % N_B, :, cols], preferred_element_type=F32)
        routed = zsum[j, :b_dev]
        wait_beside(j)
        recv_wait(zrecv.at[j], zr.at[j, 1])
        routed = routed + zside[j, :b_dev] + zrecv[j]
        y_ref[:, cols] = (h1_ref[:, cols].astype(F32) + s + routed).astype(BF16)

    for d in range(1, n):
        meta_copy(d).wait_send()
    for k, z in enumerate(others):
        u_copy(k, on(z)).wait_send()
        fwd_copy(z).wait_send()
    u_copy(nz - 1, dev(mate)).wait_send()

    @pl.loop(0, n_ch)
    def _(j):
        p_copy(j).wait_send()

        @pl.when(inner)
        def _():
            to_beside(j, 1).wait_send()
            to_other(j, 0, across).wait_send()
            to_other(j, 1, far).wait_send()

        @pl.when(jnp.logical_not(inner))
        def _():
            to_beside(j, nz - 1).wait_send()


def moe(n, u, h1, meta, eg, eu, ed, sg, su, sd, cap):
    b_dev, hid = u.shape
    e_loc, _, inter = eg.shape
    n_tok = n * b_dev
    slots = e_loc * cap
    nz = n // 2
    half = nz * b_dev
    n_ch = hid // CW
    dma = pltpu.SemaphoreType.DMA
    vm = pl.BlockSpec(memory_space=pltpu.VMEM)
    anys = pl.BlockSpec(memory_space=pl.ANY)
    flops = 2 * 3 * hid * inter * (slots + 2 * b_dev)
    return pl.pallas_call(
        functools.partial(moe_kernel, n, cap),
        out_shape=jax.ShapeDtypeStruct((b_dev, hid), BF16),
        in_specs=[vm, vm, vm] + [anys] * 6,
        out_specs=vm,
        scratch_shapes=[
            pltpu.VMEM((N_A, hid, inter), BF16),
            pltpu.VMEM((N_B, inter, hid), BF16),
            pltpu.VMEM((n,) + meta.shape, F32),
            pltpu.VMEM((n_tok, hid), BF16),
            pltpu.VMEM((slots, hid), BF16),
            pltpu.VMEM((slots, inter), BF16),
            pltpu.VMEM((slots, n_tok), BF16),
            pltpu.VMEM((3 * slots, n_tok), BF16),
            pltpu.VMEM((n_tok, 3 * slots), BF16),
            pltpu.VMEM((slots, CW), BF16),
            pltpu.VMEM((n_ch, half, CW), F32),
            pltpu.VMEM((n_ch, half, CW), F32),
            pltpu.VMEM((n_ch, half, CW), F32),
            pltpu.VMEM((n_ch, half, CW), F32),
            pltpu.VMEM((n_ch, (nz - 1) * b_dev, CW), F32),
            pltpu.VMEM((n_ch, b_dev, CW), F32),
            pltpu.VMEM((b_dev, 2 * inter), BF16),
            dma((N_A,)), dma((N_B,)),
            dma((n - 1,)), dma((n - 1,)),
            dma((nz,)), dma((nz + 1,)),
            dma((nz,)), dma((nz,)),
            dma((n_ch,)), dma((n_ch,)),
            dma((n_ch, 3)), dma((n_ch, 2)),
        ],
        compiler_params=pltpu.CompilerParams(
            collective_id=0, has_side_effects=True, vmem_limit_bytes=63 << 20),
        cost_estimate=pl.CostEstimate(flops=flops, bytes_accessed=30 * hid * inter * 2, transcendentals=0),
        name="moe",
    )(u, h1, meta, eg, eu, ed, sg, su, sd)


def solution(mesh):
    n = mesh.shape['ep']
    tok_spec = P(('rep', 'ep'))
    row_spec = P(('rep', 'ep'), None)
    cache_spec = P(('rep', 'ep'), None, None)
    exp_spec = P('ep', None, None)

    def local(x, cache, lens, ids, rw, w_q, w_dkv, w_uk, w_uv, w_o, s_gate, s_up, s_down, e_gate, e_up, e_down):
        b_dev, top = ids.shape
        e_loc = e_gate.shape[0]
        n_exp = e_loc * n
        cape = (CAP_FACTOR * b_dev * top + n_exp - 1) // n_exp
        h1, u, kv_new, meta = attention(n, x, cache, lens, ids, rw, w_q, w_dkv, w_uk, w_uv, w_o)
        y = moe(n, u, h1, meta, e_gate, e_up, e_down, s_gate, s_up, s_down, n * cape)
        return y, kv_new

    in_specs = (row_spec, cache_spec, tok_spec, row_spec, row_spec) + (P(),) * 8 + (exp_spec,) * 3
    return jax.shard_map(local, mesh=mesh, in_specs=in_specs, out_specs=(row_spec, row_spec), check_vma=False)
```

```python
import functools
import math

import jax
import jax.numpy as jnp
from jax import lax
from jax.experimental import pallas as pl
from jax.experimental.pallas import tpu as pltpu
from jax.sharding import PartitionSpec as P

EPS = 1e-6
ROPE_BASE = 1.0e4
CAP_FACTOR = 2
N_A = 6
N_B = 2
CW = 256
F32 = jnp.float32
BF16 = jnp.bfloat16


def attn_kernel(x_in, lrow_in, lens_in, ids_in, rw_in, wq, wdkv, wuk, wuv, wo, cache,
                h1_ref, u_ref, kvn_ref, meta_ref,
                x_ref, lrow_ref, lens_ref, ids_ref, rw_ref, wq_b, wdkv_b, wuk_b, wuv_b, wo_b, cache_b, q_s, ql_s, qr_s, kv_s, s_s, p_s, ol_s, o_s, sems):
    bsz, hid = x_in.shape
    heads, nope, kvl = wuk.shape
    kvd = wdkv.shape[0]
    rot = kvd - kvl
    l_max = cache.shape[2]
    qkd = nope + rot
    n_q = 3
    qc = wq.shape[1] // n_q
    n_c = 4
    bc = bsz // n_c
    n_o = 2
    oc = hid // n_o
    copies = []

    def start(src, dst):
        c = pltpu.make_async_copy(src, dst, sems.at[len(copies)])
        c.start()
        copies.append(c)
        return c

    c_x = start(x_in, x_ref)
    c_small = [start(a, b) for a, b in ((lrow_in, lrow_ref), (lens_in, lens_ref), (ids_in, ids_ref), (rw_in, rw_ref))]
    c_q = [start(wq.at[:, i * qc:(i + 1) * qc], wq_b.at[:, i * qc:(i + 1) * qc]) for i in range(n_q)]
    c_kv = start(wdkv, wdkv_b)
    c_uk = start(wuk, wuk_b)
    c_c = [start(cache.at[i * bc:(i + 1) * bc], cache_b.at[i * bc:(i + 1) * bc]) for i in range(n_c)]
    c_uv = start(wuv, wuv_b)
    c_o = [start(wo.at[:, i * oc:(i + 1) * oc], wo_b.at[:, i * oc:(i + 1) * oc]) for i in range(n_o)]

    c_x.wait()
    for c in c_small:
        c.wait()

    me = lax.axis_index('ep')
    n_tok = meta_ref.shape[1]
    top = ids_ref.shape[0]
    lane = lax.broadcasted_iota(jnp.int32, (top, n_tok), 1) // bsz
    meta_ref[...] = jnp.zeros_like(meta_ref)
    for r, v in enumerate((ids_ref[...].astype(F32) + 1.0, rw_ref[...])):
        v = jnp.concatenate([v] * (n_tok // bsz), axis=1)
        meta_ref[r * 8:r * 8 + top] = jnp.where(lane == me, v, 0.0)

    eye = lax.broadcasted_iota(jnp.int32, (bsz, bsz), 0) == lax.broadcasted_iota(jnp.int32, (bsz, bsz), 1)
    pos = jnp.sum(jnp.where(eye, lrow_ref[...].astype(F32), 0.0), axis=1, keepdims=True)
    half = rot // 2
    li = lax.broadcasted_iota(jnp.int32, (bsz, rot), 1)
    fi = jnp.where(li < half, li, li - half).astype(F32)
    ang = pos * jnp.exp(fi * (-2.0 / rot * math.log(ROPE_BASE)))
    cs = jnp.cos(ang)
    sn = jnp.sin(ang)
    sn = jnp.where(li < half, -sn, sn)

    def rope(v):
        return v * cs + jnp.concatenate([v[:, half:], v[:, :half]], axis=1) * sn

    def norm(v):
        return v * lax.rsqrt(jnp.mean(v * v, axis=-1, keepdims=True) + EPS)

    xn = norm(x_ref[...].astype(F32)).astype(BF16)
    for i in range(n_q):
        c_q[i].wait()
        q_s[:, i * qc:(i + 1) * qc] = jnp.dot(
            xn, wq_b[:, i * qc:(i + 1) * qc], preferred_element_type=F32).astype(BF16)
    c_kv.wait()
    kv = lax.dot_general(xn, wdkv_b[...], (((1,), (1,)), ((), ())), preferred_element_type=F32)
    kvn_ref[:, :kvl] = norm(kv[:, :kvl]).astype(BF16)
    kvn_ref[:, kvl:] = rope(kv[:, kvl:]).astype(BF16)
    kv_s[:, :kvd] = kvn_ref[...].astype(F32)
    c_uk.wait()
    for h in range(heads):
        c0 = h * qkd
        rs = slice(h * bsz, (h + 1) * bsz)
        ql = jnp.dot(q_s[:, c0:c0 + nope], wuk_b[h], preferred_element_type=F32).astype(BF16).astype(F32)
        for g in range(kvl // 128):
            ql_s[g, rs] = ql[:, g * 128:(g + 1) * 128]
        qr_s[rs, :rot] = rope(q_s[:, c0 + nope:c0 + qkd].astype(F32)).astype(BF16).astype(F32)

    col = lax.broadcasted_iota(jnp.int32, (heads, l_max), 1)
    scale = qkd ** -0.5
    unroll = 8
    for i in range(n_c):
        c_c[i].wait()

        @pl.loop(0, bc // unroll)
        def _(t):
            for k in range(unroll):
                b = i * bc + t * unroll + k
                ql = jnp.concatenate(
                    [ql_s[g, pl.ds(b, heads, stride=bsz), :] for g in range(kvl // 128)], axis=1)
                qr = qr_s[pl.ds(b, heads, stride=bsz), :][:, :rot]
                kl = kv_s[pl.ds(b, 1), :]
                s = jnp.dot(ql.astype(BF16), cache_b[b, :kvl], preferred_element_type=F32)
                s += jnp.dot(qr.astype(BF16), cache_b[b, kvl:], preferred_element_type=F32)
                s_new = jnp.sum(ql * kl[:, :kvl], axis=1, keepdims=True)
                s_new += jnp.sum(qr * kl[:, kvl:kvd], axis=1, keepdims=True)
                n_live = lens_ref[b]
                s = jnp.where(col < n_live, s, jnp.where(col == n_live, s_new, -jnp.inf)) * scale
                s_s[pl.ds(pl.multiple_of(b * heads, heads), heads)] = s

    blk = 128

    @pl.loop(0, bsz * heads // blk)
    def _(t):
        rs = pl.ds(pl.multiple_of(t * blk, blk), blk)
        s = s_s[rs]
        e = jnp.exp(s - jnp.max(s, axis=1, keepdims=True))
        p_s[rs] = (e / jnp.sum(e, axis=1, keepdims=True)).astype(BF16)

    @pl.loop(0, bsz // unroll)
    def _(t):
        for k in range(unroll):
            b = t * unroll + k
            rs = pl.ds(pl.multiple_of(b * heads, heads), heads)
            n_live = lens_ref[b]
            p = p_s[rs].astype(F32)
            p_old = jnp.where(col < n_live, p, 0.0).astype(BF16)
            p_new = jnp.sum(jnp.where(col == n_live, p, 0.0), axis=1, keepdims=True)
            o = lax.dot_general(p_old, cache_b[b, :kvl], (((1,), (1,)), ((), ())), preferred_element_type=F32)
            o += p_new * kv_s[pl.ds(b, 1), :][:, :kvl]
            o = o.astype(BF16).astype(F32)
            for g in range(kvl // 128):
                ol_s[g, rs] = o[:, g * 128:(g + 1) * 128]

    c_uv.wait()
    vh = wuv.shape[2]
    for h in range(heads):
        oh = jnp.concatenate(
            [ol_s[g, pl.ds(h, bsz, stride=heads), :] for g in range(kvl // 128)], axis=1).astype(BF16)
        o_s[:, h * vh:(h + 1) * vh] = jnp.dot(oh, wuv_b[h], preferred_element_type=F32).astype(BF16)
    sq = jnp.zeros((bsz, 1), F32)
    for i in range(n_o):
        c_o[i].wait()
        cols = slice(i * oc, (i + 1) * oc)
        a = jnp.dot(o_s[...], wo_b[:, cols], preferred_element_type=F32)
        h1 = (x_ref[:, cols].astype(F32) + a).astype(BF16)
        h1_ref[:, cols] = h1
        h1 = h1.astype(F32)
        sq += jnp.sum(h1 * h1, axis=1, keepdims=True)
    u_ref[...] = (h1_ref[...].astype(F32) * lax.rsqrt(sq / hid + EPS)).astype(BF16)


def attention(n, x, cache, lens, ids, rw, w_q, w_dkv, w_uk, w_uv, w_o):
    bsz, hid = x.shape
    heads, nope, kvl = w_uk.shape
    l_max, kvd = cache.shape[1:]
    vm = pl.BlockSpec(memory_space=pltpu.VMEM)
    anys = pl.BlockSpec(memory_space=pl.ANY)
    cache_t = jnp.swapaxes(cache, 1, 2)
    rows = bsz * heads
    weights = (w_q, w_dkv.T, w_uk, w_uv, w_o, cache_t)
    row = jax.ShapeDtypeStruct((bsz, hid), BF16)
    return pl.pallas_call(
        attn_kernel,
        out_shape=(row, row, jax.ShapeDtypeStruct((bsz, kvd), BF16), jax.ShapeDtypeStruct((16, n * bsz), F32)),
        in_specs=[anys] * 11,
        out_specs=(vm,) * 4,
        scratch_shapes=[
            pltpu.VMEM(x.shape, BF16),
            pltpu.VMEM((1, bsz), jnp.int32),
            pltpu.SMEM((bsz,), jnp.int32),
            pltpu.VMEM(ids.shape[::-1], jnp.int32),
            pltpu.VMEM(rw.shape[::-1], F32),
        ] + [pltpu.VMEM(w.shape, BF16) for w in weights] + [
            pltpu.VMEM((bsz, w_q.shape[1]), BF16),
            pltpu.VMEM((kvl // 128, rows, 128), F32),
            pltpu.VMEM((rows, 128), F32),
            pltpu.VMEM((bsz, kvl + 128), F32),
            pltpu.VMEM((rows, l_max), F32),
            pltpu.VMEM((rows, l_max), BF16),
            pltpu.VMEM((kvl // 128, rows, 128), F32),
            pltpu.VMEM((bsz, w_o.shape[0]), BF16),
            pltpu.SemaphoreType.DMA((17,)),
        ],
        compiler_params=pltpu.CompilerParams(vmem_limit_bytes=60 << 20),
        cost_estimate=pl.CostEstimate(
            flops=2 * bsz * (hid * (w_q.shape[1] + kvd + w_o.shape[0]) + heads * kvl * (2 * nope + 2 * l_max)),
            bytes_accessed=2 * sum(w.size for w in weights), transcendentals=rows * l_max),
        name="attn",
    )(x, lens.reshape(1, bsz), lens, ids.T, rw.T, *weights)


def moe_kernel(n, cap, u_in, h1_in, meta_in, eg, eu, ed, sg, su, sd, y_ref,
               u_ref, h1_ref, meta_ref, wa, wb, meta_all, u_all, xr, act, disp, comb_t, comb, rows,
               pown, psend, precv, zsum, zside, zrecv, sact,
               sem_i, sem_a, sem_b, ms, mr, us, ur, fs, fr, ps, pr, zs, zr):
    me = lax.axis_index('ep')
    nz = n // 2
    zi = me // 2
    co = lax.rem(me, 2)
    mate = zi * 2 + 1 - co
    b_dev, hid = u_ref.shape
    e_loc, _, inter = eg.shape
    slots = e_loc * cap
    n_tok = n * b_dev
    half = nz * b_dev
    n_ch = hid // CW

    def dev(d):
        return {'ep': d}

    low = zi < 2
    inner = jnp.logical_or(zi == 1, zi == 2)
    beside = jnp.where(low, 1 - zi, 5 - zi)
    across = jnp.where(low, 2, 1)
    far = jnp.where(low, 3, 0)
    others = (far, across, beside)

    def on(z):
        return dev(z * 2 + co)

    def a_copy(src, slot):
        return pltpu.make_async_copy(src, wa.at[slot], sem_a.at[slot])

    def start_gu(e, k):
        a_copy(eg.at[e], lax.rem(2 * e, N_A)).start()
        a_copy(eu.at[e], lax.rem(2 * e + 1, N_A)).start()

    def start_down(j):
        slot = lax.rem(j, N_B)
        for e in range(e_loc):
            pltpu.make_async_copy(
                ed.at[e, :, pl.ds(pl.multiple_of(j * CW, CW), CW)],
                wb.at[slot, :, pl.ds(e * CW, CW)], sem_b.at[slot]).start()

    def wait_a(slot):
        a_copy(eg.at[0], slot).wait()

    def wait_b(slot):
        pltpu.make_async_copy(sd.at[pl.ds(0, inter)], wb.at[slot], sem_b.at[slot]).wait()

    n_gu = 2 * e_loc
    sh_a = [(sg, 0), (su, 0), (sg, 1), (su, 1)]

    def start_unit_a(i):
        slot = i % N_A
        if i < n_gu:
            a_copy((eg if i % 2 == 0 else eu).at[i // 2], slot).start()
        else:
            r, h = sh_a[i - n_gu]
            a_copy(r.at[:, pl.ds(h * inter, inter)], slot).start()

    small = [pltpu.make_async_copy(src, dst, sem_i.at[i]) for i, (src, dst) in enumerate(
        ((u_in, u_ref), (meta_in, meta_ref), (h1_in, h1_ref)))]
    for c in small:
        c.start()
    for i in range(N_A):
        start_unit_a(i)
    for j in range(N_B):
        start_down(j)

    barrier = pltpu.get_barrier_semaphore()
    for d in range(1, n):
        pl.semaphore_signal(barrier, inc=1, device_id=dev(lax.rem(me + d, n)))
    for c in small:
        c.wait()
    pl.semaphore_wait(barrier, n - 1)

    def meta_copy(d):
        return pltpu.make_async_remote_copy(
            meta_ref, meta_all.at[me], ms.at[d - 1], mr.at[d - 1],
            device_id=dev(lax.rem(me + d, n)), device_id_type=pl.DeviceIdType.MESH)

    my_rows = pl.ds(pl.multiple_of(me * b_dev, b_dev), b_dev)

    def u_copy(k, target):
        return pltpu.make_async_remote_copy(
            u_ref, u_all.at[my_rows], us.at[k], ur.at[zi if k < nz - 1 else nz],
            device_id=target, device_id_type=pl.DeviceIdType.MESH)

    def u_rows(z, c):
        return u_all.at[pl.ds(pl.multiple_of((z * 2 + c) * b_dev, b_dev), b_dev)]

    def fwd_copy(z):
        r = u_rows(z, co)
        return pltpu.make_async_remote_copy(
            r, r, fs.at[z], fr.at[z],
            device_id=dev(mate), device_id_type=pl.DeviceIdType.MESH)

    def recv_wait(dst, sem):
        pltpu.make_async_remote_copy(
            dst, dst, us.at[0], sem, device_id=dev(mate),
            device_id_type=pl.DeviceIdType.MESH).wait_recv()

    for d in range(1, n):
        meta_copy(d).start()
    for k, z in enumerate(others):
        u_copy(k, on(z)).start()
    u_copy(nz - 1, dev(mate)).start()
    u_all[my_rows] = u_ref[...]

    tot = meta_ref[...]
    for d in range(1, n):
        src = lax.rem(me + n - d, n)
        recv_wait(meta_all.at[src], mr.at[d - 1])
        tot = tot + meta_all[src]
    half_m = tot.shape[0] // 2
    lane = lax.broadcasted_iota(jnp.int32, (e_loc, n_tok), 0) + (me * e_loc + 1)
    lane = lane.astype(F32)
    hit = jnp.zeros((e_loc, n_tok), F32)
    wt = jnp.zeros((e_loc, n_tok), F32)
    for k in range(half_m):
        eq = tot[k:k + 1] == lane
        hit = hit + jnp.where(eq, 1.0, 0.0)
        wt = wt + jnp.where(eq, tot[half_m + k:half_m + k + 1], 0.0)
    r0 = lax.broadcasted_iota(jnp.int32, (n_tok, n_tok), 0)
    r1 = lax.broadcasted_iota(jnp.int32, (n_tok, n_tok), 1)
    before = jnp.where(r0 < r1, 1.0, 0.0).astype(BF16)
    rank = jnp.dot(hit.astype(BF16), before, preferred_element_type=F32)
    rank = jnp.where(hit > 0.5, rank, -1.0)
    w1 = wt.astype(BF16).astype(F32)
    rest = wt - w1
    w2 = rest.astype(BF16).astype(F32)
    w3 = rest - w2
    row = lax.broadcasted_iota(jnp.int32, (cap, n_tok), 0).astype(F32)
    for e in range(e_loc):
        m = row == rank[e:e + 1]
        disp[e * cap:(e + 1) * cap] = jnp.where(m, 1.0, 0.0).astype(BF16)
        for p, w in enumerate((w1, w2, w3)):
            comb_t[p * slots + e * cap:p * slots + (e + 1) * cap] = jnp.where(m, w[e:e + 1], 0.0).astype(BF16)
    side = r0 // half
    blk = lax.rem(r0, half) // b_dev
    chip = jnp.where(blk == 0, zi, jnp.where(blk == 1, beside, jnp.where(blk == 2, across, far)))
    core = jnp.where(side == 0, co, 1 - co)
    tok = (chip * 2 + core) * b_dev + lax.rem(r0, b_dev)
    perm = jnp.where(r1 == tok, 1.0, 0.0).astype(BF16)
    comb[...] = lax.dot_general(perm, comb_t[...], (((1,), (1,)), ((), ())),
                                preferred_element_type=F32).astype(BF16)

    recv_wait(u_rows(zi, 1 - co), ur.at[nz])
    for z in (beside, across, far):
        recv_wait(u_rows(z, co), ur.at[z])
        fwd_copy(z).start()
    for z in (beside, across, far):
        recv_wait(u_rows(z, 1 - co), fr.at[z])

    @pl.loop(0, hid // 512)
    def _(i):
        cols = pl.ds(pl.multiple_of(i * 512, 512), 512)
        xr[:, cols] = jnp.dot(disp[...], u_all[:, cols], preferred_element_type=F32).astype(BF16)

    def gate_up(x, sa, sb, store):
        for c0 in range(0, inter, CW):
            c1 = min(c0 + CW, inter)
            g = jnp.dot(x, wa[sa, :, c0:c1], preferred_element_type=F32)
            v = jnp.dot(x, wa[sb, :, c0:c1], preferred_element_type=F32)
            store(c0, c1, (jax.nn.silu(g) * v).astype(BF16))

    def expert_body(e):
        sa = lax.rem(2 * e, N_A)
        sb = lax.rem(2 * e + 1, N_A)
        wait_a(sa)
        wait_a(sb)
        rs = pl.ds(pl.multiple_of(e * cap, cap), cap)

        def store(c0, c1, val):
            act[rs, c0:c1] = val

        gate_up(xr[rs, :], sa, sb, store)

    @pl.loop(0, e_loc)
    def _(e):
        expert_body(e)
        for t in range(2):
            i = 2 * e + t + N_A
            slot = lax.rem(i, N_A)

            @pl.when(jnp.logical_and(i < n_gu, lax.rem(i, 2) == 0))
            def _():
                a_copy(eg.at[lax.min(i // 2, e_loc - 1)], slot).start()

            @pl.when(jnp.logical_and(i < n_gu, lax.rem(i, 2) == 1))
            def _():
                a_copy(eu.at[lax.min(i // 2, e_loc - 1)], slot).start()


    def p_copy(j):
        return pltpu.make_async_remote_copy(
            psend.at[j], precv.at[j], ps.at[j], pr.at[j],
            device_id=dev(mate), device_id_type=pl.DeviceIdType.MESH)

    def to_beside(j, size):
        return pltpu.make_async_remote_copy(
            zsum.at[j, pl.ds(b_dev, size * b_dev)], zside.at[j, pl.ds(0, size * b_dev)],
            zs.at[j, 0], zr.at[j, 0], device_id=on(beside), device_id_type=pl.DeviceIdType.MESH)

    def to_other(j, k, z):
        return pltpu.make_async_remote_copy(
            zsum.at[j, pl.ds((2 + k) * b_dev, b_dev)], zrecv.at[j],
            zs.at[j, 1 + k], zr.at[j, 1], device_id=on(z), device_id_type=pl.DeviceIdType.MESH)

    def chip_sum(j):
        recv_wait(precv.at[j], pr.at[j])
        zsum[j] = pown[j] + precv[j]

        @pl.when(inner)
        def _():
            to_beside(j, 1).start()

        @pl.when(jnp.logical_not(inner))
        def _():
            to_beside(j, nz - 1).start()

    def wait_beside(j):
        @pl.when(jnp.logical_not(inner))
        def _():
            recv_wait(zside.at[j, pl.ds(0, b_dev)], zr.at[j, 0])

    def relay(j):
        @pl.when(inner)
        def _():
            recv_wait(zside.at[j], zr.at[j, 0])
            zsum[j, 2 * b_dev:] = zsum[j, 2 * b_dev:] + zside[j, b_dev:]
            to_other(j, 1, far).start()
            to_other(j, 0, across).start()

    @pl.loop(0, n_ch)
    def _(j):
        slot = lax.rem(j, N_B)
        wait_b(slot)
        for e in range(e_loc):
            rows[e * cap:(e + 1) * cap] = jnp.dot(
                act[e * cap:(e + 1) * cap], wb[slot, :, e * CW:(e + 1) * CW],
                preferred_element_type=F32).astype(BF16)

        @pl.when(j + N_B < n_ch)
        def _():
            start_down(lax.min(j + N_B, n_ch - 1))

        for h in range(2):
            i = n_ch + h

            @pl.when(j + N_B == i)
            def _():
                pltpu.make_async_copy(sd.at[pl.ds(h * inter, inter)], wb.at[i % N_B], sem_b.at[i % N_B]).start()

        @pl.when(j + N_B == n_ch - 1)
        def _():
            for i in range(n_gu, n_gu + len(sh_a)):
                start_unit_a(i)

        part = jnp.dot(comb[:, 0:slots], rows[...], preferred_element_type=F32)
        part += jnp.dot(comb[:, slots:2 * slots], rows[...], preferred_element_type=F32)
        part += jnp.dot(comb[:, 2 * slots:3 * slots], rows[...], preferred_element_type=F32)
        pown[j] = part[:half]
        psend[j] = part[half:]
        p_copy(j).start()

        @pl.when(j > 0)
        def _():
            chip_sum(lax.max(j - 1, 0))

        @pl.when(j > 1)
        def _():
            relay(lax.max(j - 2, 0))

    chip_sum(n_ch - 1)
    relay(n_ch - 2)

    for h in range(2):
        sa = (n_gu + 2 * h) % N_A
        sb = (n_gu + 2 * h + 1) % N_A
        wait_a(sa)
        wait_a(sb)

        def store(c0, c1, val):
            sact[:, h * inter + c0:h * inter + c1] = val

        gate_up(u_ref[...], sa, sb, store)
        if h == 0:
            relay(n_ch - 1)
    for h in range(2):
        wait_b((n_ch + h) % N_B)

    for j in range(n_ch):
        cols = slice(j * CW, (j + 1) * CW)
        s = jnp.dot(sact[:, :inter], wb[n_ch % N_B, :, cols], preferred_element_type=F32)
        s += jnp.dot(sact[:, inter:], wb[(n_ch + 1) % N_B, :, cols], preferred_element_type=F32)
        routed = zsum[j, :b_dev]
        wait_beside(j)
        recv_wait(zrecv.at[j], zr.at[j, 1])
        routed = routed + zside[j, :b_dev] + zrecv[j]
        y_ref[:, cols] = (h1_ref[:, cols].astype(F32) + s + routed).astype(BF16)

    for d in range(1, n):
        meta_copy(d).wait_send()
    for k, z in enumerate(others):
        u_copy(k, on(z)).wait_send()
        fwd_copy(z).wait_send()
    u_copy(nz - 1, dev(mate)).wait_send()

    @pl.loop(0, n_ch)
    def _(j):
        p_copy(j).wait_send()

        @pl.when(inner)
        def _():
            to_beside(j, 1).wait_send()
            to_other(j, 0, across).wait_send()
            to_other(j, 1, far).wait_send()

        @pl.when(jnp.logical_not(inner))
        def _():
            to_beside(j, nz - 1).wait_send()


def moe(n, u, h1, meta, eg, eu, ed, sg, su, sd, cap):
    b_dev, hid = u.shape
    e_loc, _, inter = eg.shape
    n_tok = n * b_dev
    slots = e_loc * cap
    nz = n // 2
    half = nz * b_dev
    n_ch = hid // CW
    dma = pltpu.SemaphoreType.DMA
    vm = pl.BlockSpec(memory_space=pltpu.VMEM)
    anys = pl.BlockSpec(memory_space=pl.ANY)
    flops = 2 * 3 * hid * inter * (slots + 2 * b_dev)
    return pl.pallas_call(
        functools.partial(moe_kernel, n, cap),
        out_shape=jax.ShapeDtypeStruct((b_dev, hid), BF16),
        in_specs=[anys] * 9,
        out_specs=vm,
        scratch_shapes=[
            pltpu.VMEM(u.shape, BF16),
            pltpu.VMEM(u.shape, BF16),
            pltpu.VMEM(meta.shape, F32),
            pltpu.VMEM((N_A, hid, inter), BF16),
            pltpu.VMEM((N_B, inter, hid), BF16),
            pltpu.VMEM((n,) + meta.shape, F32),
            pltpu.VMEM((n_tok, hid), BF16),
            pltpu.VMEM((slots, hid), BF16),
            pltpu.VMEM((slots, inter), BF16),
            pltpu.VMEM((slots, n_tok), BF16),
            pltpu.VMEM((3 * slots, n_tok), BF16),
            pltpu.VMEM((n_tok, 3 * slots), BF16),
            pltpu.VMEM((slots, CW), BF16),
            pltpu.VMEM((n_ch, half, CW), F32),
            pltpu.VMEM((n_ch, half, CW), F32),
            pltpu.VMEM((n_ch, half, CW), F32),
            pltpu.VMEM((n_ch, half, CW), F32),
            pltpu.VMEM((n_ch, (nz - 1) * b_dev, CW), F32),
            pltpu.VMEM((n_ch, b_dev, CW), F32),
            pltpu.VMEM((b_dev, 2 * inter), BF16),
            dma((3,)), dma((N_A,)), dma((N_B,)),
            dma((n - 1,)), dma((n - 1,)),
            dma((nz,)), dma((nz + 1,)),
            dma((nz,)), dma((nz,)),
            dma((n_ch,)), dma((n_ch,)),
            dma((n_ch, 3)), dma((n_ch, 2)),
        ],
        compiler_params=pltpu.CompilerParams(
            collective_id=0, has_side_effects=True, vmem_limit_bytes=63 << 20),
        cost_estimate=pl.CostEstimate(flops=flops, bytes_accessed=30 * hid * inter * 2, transcendentals=0),
        name="moe",
    )(u, h1, meta, eg, eu, ed, sg, su, sd)


def solution(mesh):
    n = mesh.shape['ep']
    tok_spec = P(('rep', 'ep'))
    row_spec = P(('rep', 'ep'), None)
    cache_spec = P(('rep', 'ep'), None, None)
    exp_spec = P('ep', None, None)

    def local(x, cache, lens, ids, rw, w_q, w_dkv, w_uk, w_uv, w_o, s_gate, s_up, s_down, e_gate, e_up, e_down):
        b_dev, top = ids.shape
        e_loc = e_gate.shape[0]
        n_exp = e_loc * n
        cape = (CAP_FACTOR * b_dev * top + n_exp - 1) // n_exp
        h1, u, kv_new, meta = attention(n, x, cache, lens, ids, rw, w_q, w_dkv, w_uk, w_uv, w_o)
        y = moe(n, u, h1, meta, e_gate, e_up, e_down, s_gate, s_up, s_down, n * cape)
        return y, kv_new

    in_specs = (row_spec, cache_spec, tok_spec, row_spec, row_spec) + (P(),) * 8 + (exp_spec,) * 3
    return jax.shard_map(local, mesh=mesh, in_specs=in_specs, out_specs=(row_spec, row_spec), check_vma=False)
```

```python
import functools
import math

import jax
import jax.numpy as jnp
from jax import lax
from jax.experimental import pallas as pl
from jax.experimental.pallas import tpu as pltpu
from jax.sharding import PartitionSpec as P

EPS = 1e-6
ROPE_BASE = 1.0e4
CAP_FACTOR = 2
N_A = 6
N_B = 2
CW = 256
F32 = jnp.float32
BF16 = jnp.bfloat16


def attn_kernel(x_in, lrow_in, lens_in, ids_in, rw_in, wq, wdkv, wuk, wuv, wo, cache,
                h1_ref, u_ref, kvn_ref, meta_ref,
                x_ref, lrow_ref, lens_ref, ids_ref, rw_ref, wq_b, wdkv_b, wuk_b, wuv_b, wo_b, cache_b, q_s, ql_s, qr_s, kv_s, s_s, p_s, ol_s, o_s, sems):
    bsz, hid = x_in.shape
    heads, nope, kvl = wuk.shape
    kvd = wdkv.shape[0]
    rot = kvd - kvl
    l_max = cache.shape[2]
    qkd = nope + rot
    n_q = 3
    qc = wq.shape[1] // n_q
    n_c = 4
    bc = bsz // n_c
    n_o = 2
    oc = hid // n_o
    copies = []

    def start(src, dst):
        c = pltpu.make_async_copy(src, dst, sems.at[len(copies)])
        c.start()
        copies.append(c)
        return c

    c_x = start(x_in, x_ref)
    c_small = [start(a, b) for a, b in ((lrow_in, lrow_ref), (lens_in, lens_ref), (ids_in, ids_ref), (rw_in, rw_ref))]
    c_q = [start(wq.at[:, i * qc:(i + 1) * qc], wq_b.at[:, i * qc:(i + 1) * qc]) for i in range(n_q)]
    c_kv = start(wdkv, wdkv_b)
    c_uk = start(wuk, wuk_b)
    c_c = [start(cache.at[i * bc:(i + 1) * bc], cache_b.at[i * bc:(i + 1) * bc]) for i in range(n_c)]
    c_uv = start(wuv, wuv_b)
    c_o = [start(wo.at[:, i * oc:(i + 1) * oc], wo_b.at[:, i * oc:(i + 1) * oc]) for i in range(n_o)]

    c_x.wait()
    for c in c_small:
        c.wait()

    me = lax.axis_index('ep')
    n_tok = meta_ref.shape[1]
    top = ids_ref.shape[0]
    lane = lax.broadcasted_iota(jnp.int32, (top, n_tok), 1) // bsz
    meta_ref[...] = jnp.zeros_like(meta_ref)
    for r, v in enumerate((ids_ref[...].astype(F32) + 1.0, rw_ref[...])):
        v = jnp.concatenate([v] * (n_tok // bsz), axis=1)
        meta_ref[r * 8:r * 8 + top] = jnp.where(lane == me, v, 0.0)

    eye = lax.broadcasted_iota(jnp.int32, (bsz, bsz), 0) == lax.broadcasted_iota(jnp.int32, (bsz, bsz), 1)
    pos = jnp.sum(jnp.where(eye, lrow_ref[...].astype(F32), 0.0), axis=1, keepdims=True)
    half = rot // 2
    li = lax.broadcasted_iota(jnp.int32, (bsz, rot), 1)
    fi = jnp.where(li < half, li, li - half).astype(F32)
    ang = pos * jnp.exp(fi * (-2.0 / rot * math.log(ROPE_BASE)))
    cs = jnp.cos(ang)
    sn = jnp.sin(ang)
    sn = jnp.where(li < half, -sn, sn)

    def rope(v):
        return v * cs + jnp.concatenate([v[:, half:], v[:, :half]], axis=1) * sn

    def norm(v):
        return v * lax.rsqrt(jnp.mean(v * v, axis=-1, keepdims=True) + EPS)

    xn = norm(x_ref[...].astype(F32)).astype(BF16)
    for i in range(n_q):
        c_q[i].wait()
        q_s[:, i * qc:(i + 1) * qc] = jnp.dot(
            xn, wq_b[:, i * qc:(i + 1) * qc], preferred_element_type=F32).astype(BF16)
    c_kv.wait()
    kv = lax.dot_general(xn, wdkv_b[...], (((1,), (1,)), ((), ())), preferred_element_type=F32)
    kvn_ref[:, :kvl] = norm(kv[:, :kvl]).astype(BF16)
    kvn_ref[:, kvl:] = rope(kv[:, kvl:]).astype(BF16)
    kv_s[:, :kvd] = kvn_ref[...].astype(F32)
    c_uk.wait()
    for h in range(heads):
        c0 = h * qkd
        rs = slice(h * bsz, (h + 1) * bsz)
        ql = jnp.dot(q_s[:, c0:c0 + nope], wuk_b[h], preferred_element_type=F32).astype(BF16).astype(F32)
        for g in range(kvl // 128):
            ql_s[g, rs] = ql[:, g * 128:(g + 1) * 128]
        qr_s[rs, :rot] = rope(q_s[:, c0 + nope:c0 + qkd].astype(F32)).astype(BF16).astype(F32)

    col = lax.broadcasted_iota(jnp.int32, (heads, l_max), 1)
    scale = qkd ** -0.5
    unroll = 8
    for i in range(n_c):
        c_c[i].wait()

        @pl.loop(0, bc // unroll)
        def _(t):
            for k in range(unroll):
                b = i * bc + t * unroll + k
                ql = jnp.concatenate(
                    [ql_s[g, pl.ds(b, heads, stride=bsz), :] for g in range(kvl // 128)], axis=1)
                qr = qr_s[pl.ds(b, heads, stride=bsz), :][:, :rot]
                kl = kv_s[pl.ds(b, 1), :]
                s = jnp.dot(ql.astype(BF16), cache_b[b, :kvl], preferred_element_type=F32)
                s += jnp.dot(qr.astype(BF16), cache_b[b, kvl:], preferred_element_type=F32)
                s_new = jnp.sum(ql * kl[:, :kvl], axis=1, keepdims=True)
                s_new += jnp.sum(qr * kl[:, kvl:kvd], axis=1, keepdims=True)
                n_live = lens_ref[b]
                s = jnp.where(col < n_live, s, jnp.where(col == n_live, s_new, -jnp.inf)) * scale
                s_s[pl.ds(pl.multiple_of(b * heads, heads), heads)] = s

    blk = 128

    @pl.loop(0, bsz * heads // blk)
    def _(t):
        rs = pl.ds(pl.multiple_of(t * blk, blk), blk)
        s = s_s[rs]
        e = jnp.exp(s - jnp.max(s, axis=1, keepdims=True))
        p_s[rs] = (e / jnp.sum(e, axis=1, keepdims=True)).astype(BF16)

    @pl.loop(0, bsz // unroll)
    def _(t):
        for k in range(unroll):
            b = t * unroll + k
            rs = pl.ds(pl.multiple_of(b * heads, heads), heads)
            n_live = lens_ref[b]
            p = p_s[rs].astype(F32)
            p_old = jnp.where(col < n_live, p, 0.0).astype(BF16)
            p_new = jnp.sum(jnp.where(col == n_live, p, 0.0), axis=1, keepdims=True)
            o = lax.dot_general(p_old, cache_b[b, :kvl], (((1,), (1,)), ((), ())), preferred_element_type=F32)
            o += p_new * kv_s[pl.ds(b, 1), :][:, :kvl]
            o = o.astype(BF16).astype(F32)
            for g in range(kvl // 128):
                ol_s[g, rs] = o[:, g * 128:(g + 1) * 128]

    c_uv.wait()
    vh = wuv.shape[2]
    for h in range(heads):
        oh = jnp.concatenate(
            [ol_s[g, pl.ds(h, bsz, stride=heads), :] for g in range(kvl // 128)], axis=1).astype(BF16)
        o_s[:, h * vh:(h + 1) * vh] = jnp.dot(oh, wuv_b[h], preferred_element_type=F32).astype(BF16)
    sq = jnp.zeros((bsz, 1), F32)
    for i in range(n_o):
        c_o[i].wait()
        cols = slice(i * oc, (i + 1) * oc)
        a = jnp.dot(o_s[...], wo_b[:, cols], preferred_element_type=F32)
        h1 = (x_ref[:, cols].astype(F32) + a).astype(BF16)
        h1_ref[:, cols] = h1
        h1 = h1.astype(F32)
        sq += jnp.sum(h1 * h1, axis=1, keepdims=True)
    u_ref[...] = (h1_ref[...].astype(F32) * lax.rsqrt(sq / hid + EPS)).astype(BF16)


def attention(n, x, cache, lens, ids, rw, w_q, w_dkv, w_uk, w_uv, w_o):
    bsz, hid = x.shape
    heads, nope, kvl = w_uk.shape
    l_max, kvd = cache.shape[1:]
    vm = pl.BlockSpec(memory_space=pltpu.VMEM)
    anys = pl.BlockSpec(memory_space=pl.ANY)
    cache_t = jnp.swapaxes(cache, 1, 2)
    rows = bsz * heads
    weights = (w_q, w_dkv.T, w_uk, w_uv, w_o, cache_t)
    row = jax.ShapeDtypeStruct((bsz, hid), BF16)
    return pl.pallas_call(
        attn_kernel,
        out_shape=(row, row, jax.ShapeDtypeStruct((bsz, kvd), BF16), jax.ShapeDtypeStruct((16, n * bsz), F32)),
        in_specs=[anys] * 11,
        out_specs=(vm,) * 4,
        scratch_shapes=[
            pltpu.VMEM(x.shape, BF16),
            pltpu.VMEM((1, bsz), jnp.int32),
            pltpu.SMEM((bsz,), jnp.int32),
            pltpu.VMEM(ids.shape[::-1], jnp.int32),
            pltpu.VMEM(rw.shape[::-1], F32),
        ] + [pltpu.VMEM(w.shape, BF16) for w in weights] + [
            pltpu.VMEM((bsz, w_q.shape[1]), BF16),
            pltpu.VMEM((kvl // 128, rows, 128), F32),
            pltpu.VMEM((rows, 128), F32),
            pltpu.VMEM((bsz, kvl + 128), F32),
            pltpu.VMEM((rows, l_max), F32),
            pltpu.VMEM((rows, l_max), BF16),
            pltpu.VMEM((kvl // 128, rows, 128), F32),
            pltpu.VMEM((bsz, w_o.shape[0]), BF16),
            pltpu.SemaphoreType.DMA((17,)),
        ],
        compiler_params=pltpu.CompilerParams(vmem_limit_bytes=60 << 20),
        cost_estimate=pl.CostEstimate(
            flops=2 * bsz * (hid * (w_q.shape[1] + kvd + w_o.shape[0]) + heads * kvl * (2 * nope + 2 * l_max)),
            bytes_accessed=2 * sum(w.size for w in weights), transcendentals=rows * l_max),
        name="attn",
    )(x, lens.reshape(1, bsz), lens, ids.T, rw.T, *weights)


def moe_kernel(n, cap, u_in, h1_in, meta_in, eg, eu, ed, sg, su, sd, y_ref,
               u_ref, h1_ref, meta_ref, wa, wb, meta_all, u_all, xr, act, disp, comb_t, comb, rows,
               pown, psend, precv, zsum, zside, zrecv, sact, own,
               sem_i, sem_a, sem_b, ms, mr, us, ur, fs, fr, ps, pr, zs, zr):
    me = lax.axis_index('ep')
    nz = n // 2
    zi = me // 2
    co = lax.rem(me, 2)
    mate = zi * 2 + 1 - co
    b_dev, hid = u_ref.shape
    e_loc, _, inter = eg.shape
    slots = e_loc * cap
    n_tok = n * b_dev
    half = nz * b_dev
    n_ch = hid // CW

    def dev(d):
        return {'ep': d}

    low = zi < 2
    inner = jnp.logical_or(zi == 1, zi == 2)
    beside = jnp.where(low, 1 - zi, 5 - zi)
    across = jnp.where(low, 2, 1)
    far = jnp.where(low, 3, 0)
    others = (far, across, beside)

    def on(z):
        return dev(z * 2 + co)

    def a_copy(src, slot):
        return pltpu.make_async_copy(src, wa.at[slot], sem_a.at[slot])

    def start_gu(e, k):
        a_copy(eg.at[e], lax.rem(2 * e, N_A)).start()
        a_copy(eu.at[e], lax.rem(2 * e + 1, N_A)).start()

    def start_down(j):
        slot = lax.rem(j, N_B)
        for e in range(e_loc):
            pltpu.make_async_copy(
                ed.at[e, :, pl.ds(pl.multiple_of(j * CW, CW), CW)],
                wb.at[slot, :, pl.ds(e * CW, CW)], sem_b.at[slot]).start()

    def wait_a(slot):
        a_copy(eg.at[0], slot).wait()

    def wait_b(slot):
        pltpu.make_async_copy(sd.at[pl.ds(0, inter)], wb.at[slot], sem_b.at[slot]).wait()

    n_gu = 2 * e_loc
    sh_a = [(sg, 0), (su, 0), (sg, 1), (su, 1)]

    def start_unit_a(i):
        slot = i % N_A
        if i < n_gu:
            a_copy((eg if i % 2 == 0 else eu).at[i // 2], slot).start()
        else:
            r, h = sh_a[i - n_gu]
            a_copy(r.at[:, pl.ds(h * inter, inter)], slot).start()

    small = [pltpu.make_async_copy(src, dst, sem_i.at[i]) for i, (src, dst) in enumerate(
        ((u_in, u_ref), (meta_in, meta_ref), (h1_in, h1_ref)))]
    for c in small:
        c.start()
    for i in range(N_A):
        start_unit_a(i)
    for j in range(N_B):
        start_down(j)

    barrier = pltpu.get_barrier_semaphore()
    for d in range(1, n):
        pl.semaphore_signal(barrier, inc=1, device_id=dev(lax.rem(me + d, n)))
    for c in small:
        c.wait()
    pl.semaphore_wait(barrier, n - 1)

    def meta_copy(d):
        return pltpu.make_async_remote_copy(
            meta_ref, meta_all.at[me], ms.at[d - 1], mr.at[d - 1],
            device_id=dev(lax.rem(me + d, n)), device_id_type=pl.DeviceIdType.MESH)

    my_rows = pl.ds(pl.multiple_of(me * b_dev, b_dev), b_dev)

    def u_copy(k, target):
        return pltpu.make_async_remote_copy(
            u_ref, u_all.at[my_rows], us.at[k], ur.at[zi if k < nz - 1 else nz],
            device_id=target, device_id_type=pl.DeviceIdType.MESH)

    def u_rows(z, c):
        return u_all.at[pl.ds(pl.multiple_of((z * 2 + c) * b_dev, b_dev), b_dev)]

    def fwd_copy(z):
        r = u_rows(z, co)
        return pltpu.make_async_remote_copy(
            r, r, fs.at[z], fr.at[z],
            device_id=dev(mate), device_id_type=pl.DeviceIdType.MESH)

    def recv_wait(dst, sem):
        pltpu.make_async_remote_copy(
            dst, dst, us.at[0], sem, device_id=dev(mate),
            device_id_type=pl.DeviceIdType.MESH).wait_recv()

    for d in range(1, n):
        meta_copy(d).start()
    for k, z in enumerate(others):
        u_copy(k, on(z)).start()
    u_copy(nz - 1, dev(mate)).start()
    u_all[my_rows] = u_ref[...]

    tot = meta_ref[...]
    for d in range(1, n):
        src = lax.rem(me + n - d, n)
        recv_wait(meta_all.at[src], mr.at[d - 1])
        tot = tot + meta_all[src]
    half_m = tot.shape[0] // 2
    lane = lax.broadcasted_iota(jnp.int32, (e_loc, n_tok), 0) + (me * e_loc + 1)
    lane = lane.astype(F32)
    hit = jnp.zeros((e_loc, n_tok), F32)
    wt = jnp.zeros((e_loc, n_tok), F32)
    for k in range(half_m):
        eq = tot[k:k + 1] == lane
        hit = hit + jnp.where(eq, 1.0, 0.0)
        wt = wt + jnp.where(eq, tot[half_m + k:half_m + k + 1], 0.0)
    r0 = lax.broadcasted_iota(jnp.int32, (n_tok, n_tok), 0)
    r1 = lax.broadcasted_iota(jnp.int32, (n_tok, n_tok), 1)
    before = jnp.where(r0 < r1, 1.0, 0.0).astype(BF16)
    rank = jnp.dot(hit.astype(BF16), before, preferred_element_type=F32)
    rank = jnp.where(hit > 0.5, rank, -1.0)
    w1 = wt.astype(BF16).astype(F32)
    rest = wt - w1
    w2 = rest.astype(BF16).astype(F32)
    w3 = rest - w2
    row = lax.broadcasted_iota(jnp.int32, (cap, n_tok), 0).astype(F32)
    for e in range(e_loc):
        m = row == rank[e:e + 1]
        disp[e * cap:(e + 1) * cap] = jnp.where(m, 1.0, 0.0).astype(BF16)
        for p, w in enumerate((w1, w2, w3)):
            comb_t[p * slots + e * cap:p * slots + (e + 1) * cap] = jnp.where(m, w[e:e + 1], 0.0).astype(BF16)
    side = r0 // half
    blk = lax.rem(r0, half) // b_dev
    chip = jnp.where(blk == 0, zi, jnp.where(blk == 1, beside, jnp.where(blk == 2, across, far)))
    core = jnp.where(side == 0, co, 1 - co)
    tok = (chip * 2 + core) * b_dev + lax.rem(r0, b_dev)
    perm = jnp.where(r1 == tok, 1.0, 0.0).astype(BF16)
    comb[...] = lax.dot_general(perm, comb_t[...], (((1,), (1,)), ((), ())),
                                preferred_element_type=F32).astype(BF16)

    recv_wait(u_rows(zi, 1 - co), ur.at[nz])
    for z in (beside, across, far):
        recv_wait(u_rows(z, co), ur.at[z])
        fwd_copy(z).start()
    for z in (beside, across, far):
        recv_wait(u_rows(z, 1 - co), fr.at[z])

    @pl.loop(0, hid // 512)
    def _(i):
        cols = pl.ds(pl.multiple_of(i * 512, 512), 512)
        xr[:, cols] = jnp.dot(disp[...], u_all[:, cols], preferred_element_type=F32).astype(BF16)

    def gate_up(x, sa, sb, store):
        for c0 in range(0, inter, CW):
            c1 = min(c0 + CW, inter)
            g = jnp.dot(x, wa[sa, :, c0:c1], preferred_element_type=F32)
            v = jnp.dot(x, wa[sb, :, c0:c1], preferred_element_type=F32)
            store(c0, c1, (jax.nn.silu(g) * v).astype(BF16))

    def expert_body(e):
        sa = lax.rem(2 * e, N_A)
        sb = lax.rem(2 * e + 1, N_A)
        wait_a(sa)
        wait_a(sb)
        rs = pl.ds(pl.multiple_of(e * cap, cap), cap)

        def store(c0, c1, val):
            act[rs, c0:c1] = val

        gate_up(xr[rs, :], sa, sb, store)

    @pl.loop(0, e_loc)
    def _(e):
        expert_body(e)
        for t in range(2):
            i = 2 * e + t + N_A
            slot = lax.rem(i, N_A)

            @pl.when(jnp.logical_and(i < n_gu, lax.rem(i, 2) == 0))
            def _():
                a_copy(eg.at[lax.min(i // 2, e_loc - 1)], slot).start()

            @pl.when(jnp.logical_and(i < n_gu, lax.rem(i, 2) == 1))
            def _():
                a_copy(eu.at[lax.min(i // 2, e_loc - 1)], slot).start()

            for q in range(2):
                @pl.when(i == n_gu + q)
                def _():
                    start_unit_a(n_gu + q)

    def p_copy(j):
        return pltpu.make_async_remote_copy(
            psend.at[j], precv.at[j], ps.at[j], pr.at[j],
            device_id=dev(mate), device_id_type=pl.DeviceIdType.MESH)

    def to_beside(j, size):
        return pltpu.make_async_remote_copy(
            zsum.at[j, pl.ds(b_dev, size * b_dev)], zside.at[j, pl.ds(0, size * b_dev)],
            zs.at[j, 0], zr.at[j, 0], device_id=on(beside), device_id_type=pl.DeviceIdType.MESH)

    def to_other(j, k, z):
        return pltpu.make_async_remote_copy(
            zsum.at[j, pl.ds((2 + k) * b_dev, b_dev)], zrecv.at[j],
            zs.at[j, 1 + k], zr.at[j, 1], device_id=on(z), device_id_type=pl.DeviceIdType.MESH)

    def chip_sum(j):
        recv_wait(precv.at[j], pr.at[j])
        zsum[j] = pown[j] + precv[j]

        @pl.when(inner)
        def _():
            to_beside(j, 1).start()

        @pl.when(jnp.logical_not(inner))
        def _():
            to_beside(j, nz - 1).start()

    def wait_beside(j):
        @pl.when(jnp.logical_not(inner))
        def _():
            recv_wait(zside.at[j, pl.ds(0, b_dev)], zr.at[j, 0])

    def relay(j):
        @pl.when(inner)
        def _():
            recv_wait(zside.at[j], zr.at[j, 0])
            zsum[j, 2 * b_dev:] = zsum[j, 2 * b_dev:] + zside[j, b_dev:]
            to_other(j, 1, far).start()
            to_other(j, 0, across).start()

    @pl.loop(0, n_ch)
    def _(j):
        slot = lax.rem(j, N_B)
        wait_b(slot)
        for e in range(e_loc):
            rows[e * cap:(e + 1) * cap] = jnp.dot(
                act[e * cap:(e + 1) * cap], wb[slot, :, e * CW:(e + 1) * CW],
                preferred_element_type=F32).astype(BF16)

        @pl.when(j + N_B < n_ch)
        def _():
            start_down(lax.min(j + N_B, n_ch - 1))

        for h in range(2):
            i = n_ch + h

            @pl.when(j + N_B == i)
            def _():
                pltpu.make_async_copy(sd.at[pl.ds(h * inter, inter)], wb.at[i % N_B], sem_b.at[i % N_B]).start()

        for q in range(2):
            @pl.when(j == 2 + q)
            def _():
                start_unit_a(n_gu + 2 + q)

        part = jnp.dot(comb[:, 0:slots], rows[...], preferred_element_type=F32)
        part += jnp.dot(comb[:, slots:2 * slots], rows[...], preferred_element_type=F32)
        part += jnp.dot(comb[:, 2 * slots:3 * slots], rows[...], preferred_element_type=F32)
        pown[j] = part[:half]
        psend[j] = part[half:]
        p_copy(j).start()

        @pl.when(j > 0)
        def _():
            chip_sum(lax.max(j - 1, 0))

        for k, at in enumerate((4, 5, 7)):
            @pl.when(j == at)
            def _():
                relay(k)

    chip_sum(n_ch - 1)

    for h in range(2):
        sa = (n_gu + 2 * h) % N_A
        sb = (n_gu + 2 * h + 1) % N_A
        wait_a(sa)
        wait_a(sb)

        def store(c0, c1, val):
            sact[:, h * inter + c0:h * inter + c1] = val

        gate_up(u_ref[...], sa, sb, store)
        relay(3 + 2 * h)
        relay(4 + 2 * h)
    for h in range(2):
        wait_b((n_ch + h) % N_B)

    for j in range(n_ch):
        cols = slice(j * CW, (j + 1) * CW)
        s = jnp.dot(sact[:, :inter], wb[n_ch % N_B, :, cols], preferred_element_type=F32)
        s += jnp.dot(sact[:, inter:], wb[(n_ch + 1) % N_B, :, cols], preferred_element_type=F32)
        own[:, cols] = h1_ref[:, cols].astype(F32) + s
    relay(n_ch - 1)
    for j in range(n_ch):
        cols = slice(j * CW, (j + 1) * CW)
        wait_beside(j)
        recv_wait(zrecv.at[j], zr.at[j, 1])
        routed = zsum[j, :b_dev] + zside[j, :b_dev] + zrecv[j]
        y_ref[:, cols] = (own[:, cols] + routed).astype(BF16)

    for d in range(1, n):
        meta_copy(d).wait_send()
    for k, z in enumerate(others):
        u_copy(k, on(z)).wait_send()
        fwd_copy(z).wait_send()
    u_copy(nz - 1, dev(mate)).wait_send()

    @pl.loop(0, n_ch)
    def _(j):
        p_copy(j).wait_send()

        @pl.when(inner)
        def _():
            to_beside(j, 1).wait_send()
            to_other(j, 0, across).wait_send()
            to_other(j, 1, far).wait_send()

        @pl.when(jnp.logical_not(inner))
        def _():
            to_beside(j, nz - 1).wait_send()


def moe(n, u, h1, meta, eg, eu, ed, sg, su, sd, cap):
    b_dev, hid = u.shape
    e_loc, _, inter = eg.shape
    n_tok = n * b_dev
    slots = e_loc * cap
    nz = n // 2
    half = nz * b_dev
    n_ch = hid // CW
    dma = pltpu.SemaphoreType.DMA
    vm = pl.BlockSpec(memory_space=pltpu.VMEM)
    anys = pl.BlockSpec(memory_space=pl.ANY)
    flops = 2 * 3 * hid * inter * (slots + 2 * b_dev)
    return pl.pallas_call(
        functools.partial(moe_kernel, n, cap),
        out_shape=jax.ShapeDtypeStruct((b_dev, hid), BF16),
        in_specs=[anys] * 9,
        out_specs=vm,
        scratch_shapes=[
            pltpu.VMEM(u.shape, BF16),
            pltpu.VMEM(u.shape, BF16),
            pltpu.VMEM(meta.shape, F32),
            pltpu.VMEM((N_A, hid, inter), BF16),
            pltpu.VMEM((N_B, inter, hid), BF16),
            pltpu.VMEM((n,) + meta.shape, F32),
            pltpu.VMEM((n_tok, hid), BF16),
            pltpu.VMEM((slots, hid), BF16),
            pltpu.VMEM((slots, inter), BF16),
            pltpu.VMEM((slots, n_tok), BF16),
            pltpu.VMEM((3 * slots, n_tok), BF16),
            pltpu.VMEM((n_tok, 3 * slots), BF16),
            pltpu.VMEM((slots, CW), BF16),
            pltpu.VMEM((n_ch, half, CW), F32),
            pltpu.VMEM((n_ch, half, CW), F32),
            pltpu.VMEM((n_ch, half, CW), F32),
            pltpu.VMEM((n_ch, half, CW), F32),
            pltpu.VMEM((n_ch, (nz - 1) * b_dev, CW), F32),
            pltpu.VMEM((n_ch, b_dev, CW), F32),
            pltpu.VMEM((b_dev, 2 * inter), BF16),
            pltpu.VMEM((b_dev, hid), F32),
            dma((3,)), dma((N_A,)), dma((N_B,)),
            dma((n - 1,)), dma((n - 1,)),
            dma((nz,)), dma((nz + 1,)),
            dma((nz,)), dma((nz,)),
            dma((n_ch,)), dma((n_ch,)),
            dma((n_ch, 3)), dma((n_ch, 2)),
        ],
        compiler_params=pltpu.CompilerParams(
            collective_id=0, has_side_effects=True, vmem_limit_bytes=63 << 20),
        cost_estimate=pl.CostEstimate(flops=flops, bytes_accessed=30 * hid * inter * 2, transcendentals=0),
        name="moe",
    )(u, h1, meta, eg, eu, ed, sg, su, sd)


def solution(mesh):
    n = mesh.shape['ep']
    tok_spec = P(('rep', 'ep'))
    row_spec = P(('rep', 'ep'), None)
    cache_spec = P(('rep', 'ep'), None, None)
    exp_spec = P('ep', None, None)

    def local(x, cache, lens, ids, rw, w_q, w_dkv, w_uk, w_uv, w_o, s_gate, s_up, s_down, e_gate, e_up, e_down):
        b_dev, top = ids.shape
        e_loc = e_gate.shape[0]
        n_exp = e_loc * n
        cape = (CAP_FACTOR * b_dev * top + n_exp - 1) // n_exp
        h1, u, kv_new, meta = attention(n, x, cache, lens, ids, rw, w_q, w_dkv, w_uk, w_uv, w_o)
        y = moe(n, u, h1, meta, e_gate, e_up, e_down, s_gate, s_up, s_down, n * cape)
        return y, kv_new

    in_specs = (row_spec, cache_spec, tok_spec, row_spec, row_spec) + (P(),) * 8 + (exp_spec,) * 3
    return jax.shard_map(local, mesh=mesh, in_specs=in_specs, out_specs=(row_spec, row_spec), check_vma=False)
```

```python
import functools
import math

import jax
import jax.numpy as jnp
from jax import lax
from jax.experimental import pallas as pl
from jax.experimental.pallas import tpu as pltpu
from jax.sharding import PartitionSpec as P

EPS = 1e-6
ROPE_BASE = 1.0e4
CAP_FACTOR = 2
N_A = 6
N_B = 2
CW = 256
F32 = jnp.float32
BF16 = jnp.bfloat16


def attn_kernel(x_in, lrow_in, lens_in, ids_in, rw_in, wq, wdkv, wuk, wuv, wo, cache,
                h1_ref, u_ref, kvn_ref, meta_ref,
                x_ref, lrow_ref, lens_ref, ids_ref, rw_ref, wq_b, wdkv_b, wuk_b, wuv_b, wo_b, cache_b, q_s, ql_s, qr_s, kv_s, s_s, p_s, ol_s, o_s, sems):
    bsz, hid = x_in.shape
    heads, nope, kvl = wuk.shape
    kvd = wdkv.shape[0]
    rot = kvd - kvl
    l_max = cache.shape[2]
    qkd = nope + rot
    n_q = 3
    qc = wq.shape[1] // n_q
    n_c = 4
    bc = bsz // n_c
    n_o = 2
    oc = hid // n_o
    copies = []

    def start(src, dst):
        c = pltpu.make_async_copy(src, dst, sems.at[len(copies)])
        c.start()
        copies.append(c)
        return c

    c_x = start(x_in, x_ref)
    c_small = [start(a, b) for a, b in ((lrow_in, lrow_ref), (lens_in, lens_ref), (ids_in, ids_ref), (rw_in, rw_ref))]
    c_q = [start(wq.at[:, i * qc:(i + 1) * qc], wq_b.at[:, i * qc:(i + 1) * qc]) for i in range(n_q)]
    c_kv = start(wdkv, wdkv_b)
    c_uk = start(wuk, wuk_b)
    c_c = [start(cache.at[i * bc:(i + 1) * bc], cache_b.at[i * bc:(i + 1) * bc]) for i in range(n_c)]
    c_uv = start(wuv, wuv_b)
    c_o = [start(wo.at[:, i * oc:(i + 1) * oc], wo_b.at[:, i * oc:(i + 1) * oc]) for i in range(n_o)]

    c_x.wait()
    for c in c_small:
        c.wait()

    me = lax.axis_index('ep')
    n_tok = meta_ref.shape[1]
    top = ids_ref.shape[0]
    lane = lax.broadcasted_iota(jnp.int32, (top, n_tok), 1) // bsz
    meta_ref[...] = jnp.zeros_like(meta_ref)
    for r, v in enumerate((ids_ref[...].astype(F32) + 1.0, rw_ref[...])):
        v = jnp.concatenate([v] * (n_tok // bsz), axis=1)
        meta_ref[r * 8:r * 8 + top] = jnp.where(lane == me, v, 0.0)

    eye = lax.broadcasted_iota(jnp.int32, (bsz, bsz), 0) == lax.broadcasted_iota(jnp.int32, (bsz, bsz), 1)
    pos = jnp.sum(jnp.where(eye, lrow_ref[...].astype(F32), 0.0), axis=1, keepdims=True)
    half = rot // 2
    li = lax.broadcasted_iota(jnp.int32, (bsz, rot), 1)
    fi = jnp.where(li < half, li, li - half).astype(F32)
    ang = pos * jnp.exp(fi * (-2.0 / rot * math.log(ROPE_BASE)))
    cs = jnp.cos(ang)
    sn = jnp.sin(ang)
    sn = jnp.where(li < half, -sn, sn)

    def rope(v):
        return v * cs + jnp.concatenate([v[:, half:], v[:, :half]], axis=1) * sn

    def norm(v):
        return v * lax.rsqrt(jnp.mean(v * v, axis=-1, keepdims=True) + EPS)

    xn = norm(x_ref[...].astype(F32)).astype(BF16)
    for i in range(n_q):
        c_q[i].wait()
        q_s[:, i * qc:(i + 1) * qc] = jnp.dot(
            xn, wq_b[:, i * qc:(i + 1) * qc], preferred_element_type=F32).astype(BF16)
    c_kv.wait()
    kv = lax.dot_general(xn, wdkv_b[...], (((1,), (1,)), ((), ())), preferred_element_type=F32)
    kvn_ref[:, :kvl] = norm(kv[:, :kvl]).astype(BF16)
    kvn_ref[:, kvl:] = rope(kv[:, kvl:]).astype(BF16)
    kv_s[:, :kvd] = kvn_ref[...].astype(F32)
    c_uk.wait()
    for h in range(heads):
        c0 = h * qkd
        rs = slice(h * bsz, (h + 1) * bsz)
        ql = jnp.dot(q_s[:, c0:c0 + nope], wuk_b[h], preferred_element_type=F32).astype(BF16).astype(F32)
        for g in range(kvl // 128):
            ql_s[g, rs] = ql[:, g * 128:(g + 1) * 128]
        qr_s[rs, :rot] = rope(q_s[:, c0 + nope:c0 + qkd].astype(F32)).astype(BF16).astype(F32)

    col = lax.broadcasted_iota(jnp.int32, (heads, l_max), 1)
    scale = qkd ** -0.5
    unroll = 8
    for i in range(n_c):
        c_c[i].wait()

        @pl.loop(0, bc // unroll)
        def _(t):
            for k in range(unroll):
                b = i * bc + t * unroll + k
                ql = jnp.concatenate(
                    [ql_s[g, pl.ds(b, heads, stride=bsz), :] for g in range(kvl // 128)], axis=1)
                qr = qr_s[pl.ds(b, heads, stride=bsz), :][:, :rot]
                kl = kv_s[pl.ds(b, 1), :]
                s = jnp.dot(ql.astype(BF16), cache_b[b, :kvl], preferred_element_type=F32)
                s += jnp.dot(qr.astype(BF16), cache_b[b, kvl:], preferred_element_type=F32)
                s_new = jnp.sum(ql * kl[:, :kvl], axis=1, keepdims=True)
                s_new += jnp.sum(qr * kl[:, kvl:kvd], axis=1, keepdims=True)
                n_live = lens_ref[b]
                s = jnp.where(col < n_live, s, jnp.where(col == n_live, s_new, -jnp.inf)) * scale
                s_s[pl.ds(pl.multiple_of(b * heads, heads), heads)] = s

    blk = 128

    @pl.loop(0, bsz * heads // blk)
    def _(t):
        rs = pl.ds(pl.multiple_of(t * blk, blk), blk)
        s = s_s[rs]
        e = jnp.exp(s - jnp.max(s, axis=1, keepdims=True))
        p_s[rs] = (e / jnp.sum(e, axis=1, keepdims=True)).astype(BF16)

    @pl.loop(0, bsz // unroll)
    def _(t):
        for k in range(unroll):
            b = t * unroll + k
            rs = pl.ds(pl.multiple_of(b * heads, heads), heads)
            n_live = lens_ref[b]
            p = p_s[rs].astype(F32)
            p_old = jnp.where(col < n_live, p, 0.0).astype(BF16)
            p_new = jnp.sum(jnp.where(col == n_live, p, 0.0), axis=1, keepdims=True)
            o = lax.dot_general(p_old, cache_b[b, :kvl], (((1,), (1,)), ((), ())), preferred_element_type=F32)
            o += p_new * kv_s[pl.ds(b, 1), :][:, :kvl]
            o = o.astype(BF16).astype(F32)
            for g in range(kvl // 128):
                ol_s[g, rs] = o[:, g * 128:(g + 1) * 128]

    c_uv.wait()
    vh = wuv.shape[2]
    for h in range(heads):
        oh = jnp.concatenate(
            [ol_s[g, pl.ds(h, bsz, stride=heads), :] for g in range(kvl // 128)], axis=1).astype(BF16)
        o_s[:, h * vh:(h + 1) * vh] = jnp.dot(oh, wuv_b[h], preferred_element_type=F32).astype(BF16)
    sq = jnp.zeros((bsz, 1), F32)
    for i in range(n_o):
        c_o[i].wait()
        cols = slice(i * oc, (i + 1) * oc)
        a = jnp.dot(o_s[...], wo_b[:, cols], preferred_element_type=F32)
        h1 = (x_ref[:, cols].astype(F32) + a).astype(BF16)
        h1_ref[:, cols] = h1
        h1 = h1.astype(F32)
        sq += jnp.sum(h1 * h1, axis=1, keepdims=True)
    u_ref[...] = (h1_ref[...].astype(F32) * lax.rsqrt(sq / hid + EPS)).astype(BF16)


def attention(n, x, cache, lens, ids, rw, w_q, w_dkv, w_uk, w_uv, w_o):
    bsz, hid = x.shape
    heads, nope, kvl = w_uk.shape
    l_max, kvd = cache.shape[1:]
    vm = pl.BlockSpec(memory_space=pltpu.VMEM)
    anys = pl.BlockSpec(memory_space=pl.ANY)
    cache_t = jnp.swapaxes(cache, 1, 2)
    rows = bsz * heads
    weights = (w_q, w_dkv.T, w_uk, w_uv, w_o, cache_t)
    row = jax.ShapeDtypeStruct((bsz, hid), BF16)
    return pl.pallas_call(
        attn_kernel,
        out_shape=(row, row, jax.ShapeDtypeStruct((bsz, kvd), BF16), jax.ShapeDtypeStruct((16, n * bsz), F32)),
        in_specs=[anys] * 11,
        out_specs=(vm,) * 4,
        scratch_shapes=[
            pltpu.VMEM(x.shape, BF16),
            pltpu.VMEM((1, bsz), jnp.int32),
            pltpu.SMEM((bsz,), jnp.int32),
            pltpu.VMEM(ids.shape[::-1], jnp.int32),
            pltpu.VMEM(rw.shape[::-1], F32),
        ] + [pltpu.VMEM(w.shape, BF16) for w in weights] + [
            pltpu.VMEM((bsz, w_q.shape[1]), BF16),
            pltpu.VMEM((kvl // 128, rows, 128), F32),
            pltpu.VMEM((rows, 128), F32),
            pltpu.VMEM((bsz, kvl + 128), F32),
            pltpu.VMEM((rows, l_max), F32),
            pltpu.VMEM((rows, l_max), BF16),
            pltpu.VMEM((kvl // 128, rows, 128), F32),
            pltpu.VMEM((bsz, w_o.shape[0]), BF16),
            pltpu.SemaphoreType.DMA((17,)),
        ],
        compiler_params=pltpu.CompilerParams(vmem_limit_bytes=60 << 20),
        cost_estimate=pl.CostEstimate(
            flops=2 * bsz * (hid * (w_q.shape[1] + kvd + w_o.shape[0]) + heads * kvl * (2 * nope + 2 * l_max)),
            bytes_accessed=2 * sum(w.size for w in weights), transcendentals=rows * l_max),
        name="attn",
    )(x, lens.reshape(1, bsz), lens, ids.T, rw.T, *weights)


def moe_kernel(n, cap, u_in, h1_in, meta_in, eg, eu, ed, sg, su, sd, y_ref,
               u_ref, h1_ref, meta_ref, wa, wb, meta_all, u_all, xr, act, disp, comb_t, comb, rows,
               pown, psend, precv, zsum, zside, zrecv, sact, own,
               sem_i, sem_a, sem_b, ms, mr, us, ur, fs, fr, ps, pr, zs, zr):
    me = lax.axis_index('ep')
    nz = n // 2
    zi = me // 2
    co = lax.rem(me, 2)
    mate = zi * 2 + 1 - co
    b_dev, hid = u_ref.shape
    e_loc, _, inter = eg.shape
    slots = e_loc * cap
    n_tok = n * b_dev
    half = nz * b_dev
    n_ch = hid // CW

    def dev(d):
        return {'ep': d}

    low = zi < 2
    inner = jnp.logical_or(zi == 1, zi == 2)
    beside = jnp.where(low, 1 - zi, 5 - zi)
    across = jnp.where(low, 2, 1)
    far = jnp.where(low, 3, 0)
    others = (far, across, beside)

    def on(z):
        return dev(z * 2 + co)

    def a_copy(src, slot):
        return pltpu.make_async_copy(src, wa.at[slot], sem_a.at[slot])

    def start_down(j):
        slot = lax.rem(j, N_B)
        for e in range(e_loc):
            pltpu.make_async_copy(
                ed.at[e, :, pl.ds(pl.multiple_of(j * CW, CW), CW)],
                wb.at[slot, :, pl.ds(e * CW, CW)], sem_b.at[slot]).start()

    def wait_a(slot):
        a_copy(eg.at[0], slot).wait()

    def wait_b(slot):
        pltpu.make_async_copy(sd.at[pl.ds(0, inter)], wb.at[slot], sem_b.at[slot]).wait()

    n_gu = 2 * e_loc
    sh_a = [(sg, 0), (su, 0), (sg, 1), (su, 1)]

    def start_unit_a(i):
        slot = i % N_A
        if i < n_gu:
            a_copy((eg if i % 2 == 0 else eu).at[i // 2], slot).start()
        else:
            r, h = sh_a[i - n_gu]
            a_copy(r.at[:, pl.ds(h * inter, inter)], slot).start()

    small = [pltpu.make_async_copy(src, dst, sem_i.at[i]) for i, (src, dst) in enumerate(
        ((u_in, u_ref), (meta_in, meta_ref), (h1_in, h1_ref)))]
    for c in small:
        c.start()
    barrier = pltpu.get_barrier_semaphore()
    for d in range(1, n):
        pl.semaphore_signal(barrier, inc=1, device_id=dev(lax.rem(me + d, n)))
    for c in small:
        c.wait()
    pl.semaphore_wait(barrier, n - 1)

    def meta_copy(d):
        return pltpu.make_async_remote_copy(
            meta_ref, meta_all.at[me], ms.at[d - 1], mr.at[d - 1],
            device_id=dev(lax.rem(me + d, n)), device_id_type=pl.DeviceIdType.MESH)

    my_rows = pl.ds(pl.multiple_of(me * b_dev, b_dev), b_dev)

    def u_copy(k, target):
        return pltpu.make_async_remote_copy(
            u_ref, u_all.at[my_rows], us.at[k], ur.at[zi if k < nz - 1 else nz],
            device_id=target, device_id_type=pl.DeviceIdType.MESH)

    def u_rows(z, c):
        return u_all.at[pl.ds(pl.multiple_of((z * 2 + c) * b_dev, b_dev), b_dev)]

    def fwd_copy(z):
        r = u_rows(z, co)
        return pltpu.make_async_remote_copy(
            r, r, fs.at[z], fr.at[z],
            device_id=dev(mate), device_id_type=pl.DeviceIdType.MESH)

    def recv_wait(dst, sem):
        pltpu.make_async_remote_copy(
            dst, dst, us.at[0], sem, device_id=dev(mate),
            device_id_type=pl.DeviceIdType.MESH).wait_recv()

    for d in range(1, n):
        meta_copy(d).start()
    for k, z in enumerate(others):
        u_copy(k, on(z)).start()
    u_copy(nz - 1, dev(mate)).start()
    for i in range(N_A):
        start_unit_a(i)
    u_all[my_rows] = u_ref[...]

    tot = meta_ref[...]
    for d in range(1, n):
        src = lax.rem(me + n - d, n)
        recv_wait(meta_all.at[src], mr.at[d - 1])
        tot = tot + meta_all[src]
    half_m = tot.shape[0] // 2
    lane = lax.broadcasted_iota(jnp.int32, (e_loc, n_tok), 0) + (me * e_loc + 1)
    lane = lane.astype(F32)
    hit = jnp.zeros((e_loc, n_tok), F32)
    wt = jnp.zeros((e_loc, n_tok), F32)
    for k in range(half_m):
        eq = tot[k:k + 1] == lane
        hit = hit + jnp.where(eq, 1.0, 0.0)
        wt = wt + jnp.where(eq, tot[half_m + k:half_m + k + 1], 0.0)
    r0 = lax.broadcasted_iota(jnp.int32, (n_tok, n_tok), 0)
    r1 = lax.broadcasted_iota(jnp.int32, (n_tok, n_tok), 1)
    before = jnp.where(r0 < r1, 1.0, 0.0).astype(BF16)
    rank = jnp.dot(hit.astype(BF16), before, preferred_element_type=F32)
    rank = jnp.where(hit > 0.5, rank, -1.0)
    w1 = wt.astype(BF16).astype(F32)
    rest = wt - w1
    w2 = rest.astype(BF16).astype(F32)
    w3 = rest - w2
    row = lax.broadcasted_iota(jnp.int32, (cap, n_tok), 0).astype(F32)
    for e in range(e_loc):
        m = row == rank[e:e + 1]
        disp[e * cap:(e + 1) * cap] = jnp.where(m, 1.0, 0.0).astype(BF16)
        for p, w in enumerate((w1, w2, w3)):
            comb_t[p * slots + e * cap:p * slots + (e + 1) * cap] = jnp.where(m, w[e:e + 1], 0.0).astype(BF16)
    side = r0 // half
    blk = lax.rem(r0, half) // b_dev
    chip = jnp.where(blk == 0, zi, jnp.where(blk == 1, beside, jnp.where(blk == 2, across, far)))
    core = jnp.where(side == 0, co, 1 - co)
    tok = (chip * 2 + core) * b_dev + lax.rem(r0, b_dev)
    perm = jnp.where(r1 == tok, 1.0, 0.0).astype(BF16)
    comb[...] = lax.dot_general(perm, comb_t[...], (((1,), (1,)), ((), ())),
                                preferred_element_type=F32).astype(BF16)

    recv_wait(u_rows(zi, 1 - co), ur.at[nz])
    for z in (beside, across, far):
        recv_wait(u_rows(z, co), ur.at[z])
        fwd_copy(z).start()
    for z in (beside, across, far):
        recv_wait(u_rows(z, 1 - co), fr.at[z])

    for j in range(N_B):
        start_down(j)

    @pl.loop(0, hid // 512)
    def _(i):
        cols = pl.ds(pl.multiple_of(i * 512, 512), 512)
        xr[:, cols] = jnp.dot(disp[...], u_all[:, cols], preferred_element_type=F32).astype(BF16)

    def gate_up(x, sa, sb, store):
        for c0 in range(0, inter, CW):
            c1 = min(c0 + CW, inter)
            g = jnp.dot(x, wa[sa, :, c0:c1], preferred_element_type=F32)
            v = jnp.dot(x, wa[sb, :, c0:c1], preferred_element_type=F32)
            store(c0, c1, (jax.nn.silu(g) * v).astype(BF16))

    def expert_body(e):
        sa = lax.rem(2 * e, N_A)
        sb = lax.rem(2 * e + 1, N_A)
        wait_a(sa)
        wait_a(sb)
        rs = pl.ds(pl.multiple_of(e * cap, cap), cap)

        def store(c0, c1, val):
            act[rs, c0:c1] = val

        gate_up(xr[rs, :], sa, sb, store)

    @pl.loop(0, e_loc)
    def _(e):
        expert_body(e)
        for t in range(2):
            i = 2 * e + t + N_A
            slot = lax.rem(i, N_A)

            @pl.when(jnp.logical_and(i < n_gu, lax.rem(i, 2) == 0))
            def _():
                a_copy(eg.at[lax.min(i // 2, e_loc - 1)], slot).start()

            @pl.when(jnp.logical_and(i < n_gu, lax.rem(i, 2) == 1))
            def _():
                a_copy(eu.at[lax.min(i // 2, e_loc - 1)], slot).start()

            for q in range(2):
                @pl.when(i == n_gu + q)
                def _():
                    start_unit_a(n_gu + q)

    def p_copy(j):
        return pltpu.make_async_remote_copy(
            psend.at[j], precv.at[j], ps.at[j], pr.at[j],
            device_id=dev(mate), device_id_type=pl.DeviceIdType.MESH)

    def to_beside(j, size):
        return pltpu.make_async_remote_copy(
            zsum.at[j, pl.ds(b_dev, size * b_dev)], zside.at[j, pl.ds(0, size * b_dev)],
            zs.at[j, 0], zr.at[j, 0], device_id=on(beside), device_id_type=pl.DeviceIdType.MESH)

    def to_other(j, k, z):
        return pltpu.make_async_remote_copy(
            zsum.at[j, pl.ds((2 + k) * b_dev, b_dev)], zrecv.at[j],
            zs.at[j, 1 + k], zr.at[j, 1], device_id=on(z), device_id_type=pl.DeviceIdType.MESH)

    def chip_sum(j):
        recv_wait(precv.at[j], pr.at[j])
        zsum[j] = pown[j] + precv[j]

        @pl.when(inner)
        def _():
            to_beside(j, 1).start()

        @pl.when(jnp.logical_not(inner))
        def _():
            to_beside(j, nz - 1).start()

    def wait_beside(j):
        @pl.when(jnp.logical_not(inner))
        def _():
            recv_wait(zside.at[j, pl.ds(0, b_dev)], zr.at[j, 0])

    def relay(j):
        @pl.when(inner)
        def _():
            recv_wait(zside.at[j], zr.at[j, 0])
            zsum[j, 2 * b_dev:] = zsum[j, 2 * b_dev:] + zside[j, b_dev:]
            to_other(j, 1, far).start()
            to_other(j, 0, across).start()

    @pl.loop(0, n_ch)
    def _(j):
        slot = lax.rem(j, N_B)
        wait_b(slot)
        for e in range(e_loc):
            rows[e * cap:(e + 1) * cap] = jnp.dot(
                act[e * cap:(e + 1) * cap], wb[slot, :, e * CW:(e + 1) * CW],
                preferred_element_type=F32).astype(BF16)

        part = jnp.dot(comb[:, 0:slots], rows[...], preferred_element_type=F32)
        part += jnp.dot(comb[:, slots:2 * slots], rows[...], preferred_element_type=F32)
        part += jnp.dot(comb[:, 2 * slots:3 * slots], rows[...], preferred_element_type=F32)
        pown[j] = part[:half]
        psend[j] = part[half:]
        p_copy(j).start()

        @pl.when(j > 1)
        def _():
            chip_sum(lax.max(j - 2, 0))

        @pl.when(j > 4)
        def _():
            relay(lax.max(j - 5, 0))

        @pl.when(j + N_B < n_ch)
        def _():
            start_down(lax.min(j + N_B, n_ch - 1))

        for h in range(2):
            i = n_ch + h

            @pl.when(j + N_B == i)
            def _():
                pltpu.make_async_copy(sd.at[pl.ds(h * inter, inter)], wb.at[i % N_B], sem_b.at[i % N_B]).start()

        @pl.when(j + N_B == n_ch - 1)
        def _():
            for q in range(2):
                start_unit_a(n_gu + 2 + q)

    chip_sum(n_ch - 2)
    chip_sum(n_ch - 1)
    relay(n_ch - 5)

    for h in range(2):
        sa = (n_gu + 2 * h) % N_A
        sb = (n_gu + 2 * h + 1) % N_A
        wait_a(sa)
        wait_a(sb)

        def store(c0, c1, val):
            sact[:, h * inter + c0:h * inter + c1] = val

        gate_up(u_ref[...], sa, sb, store)
        relay(n_ch - 4 + 2 * h)
        relay(n_ch - 3 + 2 * h)
    for h in range(2):
        wait_b((n_ch + h) % N_B)

    for j in range(n_ch):
        cols = slice(j * CW, (j + 1) * CW)
        s = jnp.dot(sact[:, :inter], wb[n_ch % N_B, :, cols], preferred_element_type=F32)
        s += jnp.dot(sact[:, inter:], wb[(n_ch + 1) % N_B, :, cols], preferred_element_type=F32)
        own[:, cols] = h1_ref[:, cols].astype(F32) + s
    for j in range(n_ch):
        cols = slice(j * CW, (j + 1) * CW)
        wait_beside(j)
        recv_wait(zrecv.at[j], zr.at[j, 1])
        routed = zsum[j, :b_dev] + zside[j, :b_dev] + zrecv[j]
        y_ref[:, cols] = (own[:, cols] + routed).astype(BF16)

    for d in range(1, n):
        meta_copy(d).wait_send()
    for k, z in enumerate(others):
        u_copy(k, on(z)).wait_send()
        fwd_copy(z).wait_send()
    u_copy(nz - 1, dev(mate)).wait_send()

    @pl.loop(0, n_ch)
    def _(j):
        p_copy(j).wait_send()

        @pl.when(inner)
        def _():
            to_beside(j, 1).wait_send()
            to_other(j, 0, across).wait_send()
            to_other(j, 1, far).wait_send()

        @pl.when(jnp.logical_not(inner))
        def _():
            to_beside(j, nz - 1).wait_send()


def moe(n, u, h1, meta, eg, eu, ed, sg, su, sd, cap):
    b_dev, hid = u.shape
    e_loc, _, inter = eg.shape
    n_tok = n * b_dev
    slots = e_loc * cap
    nz = n // 2
    half = nz * b_dev
    n_ch = hid // CW
    dma = pltpu.SemaphoreType.DMA
    vm = pl.BlockSpec(memory_space=pltpu.VMEM)
    anys = pl.BlockSpec(memory_space=pl.ANY)
    flops = 2 * 3 * hid * inter * (slots + 2 * b_dev)
    return pl.pallas_call(
        functools.partial(moe_kernel, n, cap),
        out_shape=jax.ShapeDtypeStruct((b_dev, hid), BF16),
        in_specs=[anys] * 9,
        out_specs=vm,
        scratch_shapes=[
            pltpu.VMEM(u.shape, BF16),
            pltpu.VMEM(u.shape, BF16),
            pltpu.VMEM(meta.shape, F32),
            pltpu.VMEM((N_A, hid, inter), BF16),
            pltpu.VMEM((N_B, inter, hid), BF16),
            pltpu.VMEM((n,) + meta.shape, F32),
            pltpu.VMEM((n_tok, hid), BF16),
            pltpu.VMEM((slots, hid), BF16),
            pltpu.VMEM((slots, inter), BF16),
            pltpu.VMEM((slots, n_tok), BF16),
            pltpu.VMEM((3 * slots, n_tok), BF16),
            pltpu.VMEM((n_tok, 3 * slots), BF16),
            pltpu.VMEM((slots, CW), BF16),
            pltpu.VMEM((n_ch, half, CW), F32),
            pltpu.VMEM((n_ch, half, CW), F32),
            pltpu.VMEM((n_ch, half, CW), F32),
            pltpu.VMEM((n_ch, half, CW), F32),
            pltpu.VMEM((n_ch, (nz - 1) * b_dev, CW), F32),
            pltpu.VMEM((n_ch, b_dev, CW), F32),
            pltpu.VMEM((b_dev, 2 * inter), BF16),
            pltpu.VMEM((b_dev, hid), F32),
            dma((3,)), dma((N_A,)), dma((N_B,)),
            dma((n - 1,)), dma((n - 1,)),
            dma((nz,)), dma((nz + 1,)),
            dma((nz,)), dma((nz,)),
            dma((n_ch,)), dma((n_ch,)),
            dma((n_ch, 3)), dma((n_ch, 2)),
        ],
        compiler_params=pltpu.CompilerParams(
            collective_id=0, has_side_effects=True, vmem_limit_bytes=63 << 20),
        cost_estimate=pl.CostEstimate(flops=flops, bytes_accessed=30 * hid * inter * 2, transcendentals=0),
        name="moe",
    )(u, h1, meta, eg, eu, ed, sg, su, sd)


def solution(mesh):
    n = mesh.shape['ep']
    tok_spec = P(('rep', 'ep'))
    row_spec = P(('rep', 'ep'), None)
    cache_spec = P(('rep', 'ep'), None, None)
    exp_spec = P('ep', None, None)

    def local(x, cache, lens, ids, rw, w_q, w_dkv, w_uk, w_uv, w_o, s_gate, s_up, s_down, e_gate, e_up, e_down):
        b_dev, top = ids.shape
        e_loc = e_gate.shape[0]
        n_exp = e_loc * n
        cape = (CAP_FACTOR * b_dev * top + n_exp - 1) // n_exp
        h1, u, kv_new, meta = attention(n, x, cache, lens, ids, rw, w_q, w_dkv, w_uk, w_uv, w_o)
        y = moe(n, u, h1, meta, e_gate, e_up, e_down, s_gate, s_up, s_down, n * cape)
        return y, kv_new

    in_specs = (row_spec, cache_spec, tok_spec, row_spec, row_spec) + (P(),) * 8 + (exp_spec,) * 3
    return jax.shard_map(local, mesh=mesh, in_specs=in_specs, out_specs=(row_spec, row_spec), check_vma=False)
```

```python
import functools
import math

import jax
import jax.numpy as jnp
from jax import lax
from jax.experimental import pallas as pl
from jax.experimental.pallas import tpu as pltpu
from jax.sharding import PartitionSpec as P

EPS = 1e-6
ROPE_BASE = 1.0e4
CAP_FACTOR = 2
N_A = 5
N_B = 3
CW = 256
F32 = jnp.float32
BF16 = jnp.bfloat16


def attn_kernel(x_in, lrow_in, lens_in, ids_in, rw_in, wq, wdkv, wuk, wuv, wo, cache,
                h1_ref, u_ref, kvn_ref, meta_ref,
                x_ref, lrow_ref, lens_ref, ids_ref, rw_ref, wq_b, wdkv_b, wuk_b, wuv_b, wo_b, cache_b, q_s, ql_s, qr_s, kv_s, s_s, p_s, ol_s, o_s, sems):
    bsz, hid = x_in.shape
    heads, nope, kvl = wuk.shape
    kvd = wdkv.shape[0]
    rot = kvd - kvl
    l_max = cache.shape[2]
    qkd = nope + rot
    n_q = 3
    qc = wq.shape[1] // n_q
    n_c = 4
    bc = bsz // n_c
    n_o = 2
    oc = hid // n_o
    copies = []

    def start(src, dst):
        c = pltpu.make_async_copy(src, dst, sems.at[len(copies)])
        c.start()
        copies.append(c)
        return c

    c_x = start(x_in, x_ref)
    c_small = [start(a, b) for a, b in ((lrow_in, lrow_ref), (lens_in, lens_ref), (ids_in, ids_ref), (rw_in, rw_ref))]
    c_q = [start(wq.at[:, i * qc:(i + 1) * qc], wq_b.at[:, i * qc:(i + 1) * qc]) for i in range(n_q)]
    c_kv = start(wdkv, wdkv_b)
    c_uk = start(wuk, wuk_b)
    c_c = [start(cache.at[i * bc:(i + 1) * bc], cache_b.at[i * bc:(i + 1) * bc]) for i in range(n_c)]
    c_uv = start(wuv, wuv_b)
    c_o = [start(wo.at[:, i * oc:(i + 1) * oc], wo_b.at[:, i * oc:(i + 1) * oc]) for i in range(n_o)]

    c_x.wait()
    for c in c_small:
        c.wait()

    me = lax.axis_index('ep')
    n_tok = meta_ref.shape[1]
    top = ids_ref.shape[0]
    lane = lax.broadcasted_iota(jnp.int32, (top, n_tok), 1) // bsz
    meta_ref[...] = jnp.zeros_like(meta_ref)
    for r, v in enumerate((ids_ref[...].astype(F32) + 1.0, rw_ref[...])):
        v = jnp.concatenate([v] * (n_tok // bsz), axis=1)
        meta_ref[r * 8:r * 8 + top] = jnp.where(lane == me, v, 0.0)

    eye = lax.broadcasted_iota(jnp.int32, (bsz, bsz), 0) == lax.broadcasted_iota(jnp.int32, (bsz, bsz), 1)
    pos = jnp.sum(jnp.where(eye, lrow_ref[...].astype(F32), 0.0), axis=1, keepdims=True)
    half = rot // 2
    li = lax.broadcasted_iota(jnp.int32, (bsz, rot), 1)
    fi = jnp.where(li < half, li, li - half).astype(F32)
    ang = pos * jnp.exp(fi * (-2.0 / rot * math.log(ROPE_BASE)))
    cs = jnp.cos(ang)
    sn = jnp.sin(ang)
    sn = jnp.where(li < half, -sn, sn)

    def rope(v):
        return v * cs + jnp.concatenate([v[:, half:], v[:, :half]], axis=1) * sn

    def norm(v):
        return v * lax.rsqrt(jnp.mean(v * v, axis=-1, keepdims=True) + EPS)

    xn = norm(x_ref[...].astype(F32)).astype(BF16)
    for i in range(n_q):
        c_q[i].wait()
        q_s[:, i * qc:(i + 1) * qc] = jnp.dot(
            xn, wq_b[:, i * qc:(i + 1) * qc], preferred_element_type=F32).astype(BF16)
    c_kv.wait()
    kv = lax.dot_general(xn, wdkv_b[...], (((1,), (1,)), ((), ())), preferred_element_type=F32)
    kvn_ref[:, :kvl] = norm(kv[:, :kvl]).astype(BF16)
    kvn_ref[:, kvl:] = rope(kv[:, kvl:]).astype(BF16)
    kv_s[:, :kvd] = kvn_ref[...].astype(F32)
    c_uk.wait()
    for h in range(heads):
        c0 = h * qkd
        rs = slice(h * bsz, (h + 1) * bsz)
        ql = jnp.dot(q_s[:, c0:c0 + nope], wuk_b[h], preferred_element_type=F32).astype(BF16).astype(F32)
        for g in range(kvl // 128):
            ql_s[g, rs] = ql[:, g * 128:(g + 1) * 128]
        qr_s[rs, :rot] = rope(q_s[:, c0 + nope:c0 + qkd].astype(F32)).astype(BF16).astype(F32)

    col = lax.broadcasted_iota(jnp.int32, (heads, l_max), 1)
    scale = qkd ** -0.5
    unroll = 8
    for i in range(n_c):
        c_c[i].wait()

        @pl.loop(0, bc // unroll)
        def _(t):
            for k in range(unroll):
                b = i * bc + t * unroll + k
                ql = jnp.concatenate(
                    [ql_s[g, pl.ds(b, heads, stride=bsz), :] for g in range(kvl // 128)], axis=1)
                qr = qr_s[pl.ds(b, heads, stride=bsz), :][:, :rot]
                kl = kv_s[pl.ds(b, 1), :]
                s = jnp.dot(ql.astype(BF16), cache_b[b, :kvl], preferred_element_type=F32)
                s += jnp.dot(qr.astype(BF16), cache_b[b, kvl:], preferred_element_type=F32)
                s_new = jnp.sum(ql * kl[:, :kvl], axis=1, keepdims=True)
                s_new += jnp.sum(qr * kl[:, kvl:kvd], axis=1, keepdims=True)
                n_live = lens_ref[b]
                s = jnp.where(col < n_live, s, jnp.where(col == n_live, s_new, -jnp.inf)) * scale
                s_s[pl.ds(pl.multiple_of(b * heads, heads), heads)] = s

    blk = 128

    @pl.loop(0, bsz * heads // blk)
    def _(t):
        rs = pl.ds(pl.multiple_of(t * blk, blk), blk)
        s = s_s[rs]
        e = jnp.exp(s - jnp.max(s, axis=1, keepdims=True))
        p_s[rs] = (e / jnp.sum(e, axis=1, keepdims=True)).astype(BF16)

    @pl.loop(0, bsz // unroll)
    def _(t):
        for k in range(unroll):
            b = t * unroll + k
            rs = pl.ds(pl.multiple_of(b * heads, heads), heads)
            n_live = lens_ref[b]
            p = p_s[rs].astype(F32)
            p_old = jnp.where(col < n_live, p, 0.0).astype(BF16)
            p_new = jnp.sum(jnp.where(col == n_live, p, 0.0), axis=1, keepdims=True)
            o = lax.dot_general(p_old, cache_b[b, :kvl], (((1,), (1,)), ((), ())), preferred_element_type=F32)
            o += p_new * kv_s[pl.ds(b, 1), :][:, :kvl]
            o = o.astype(BF16).astype(F32)
            for g in range(kvl // 128):
                ol_s[g, rs] = o[:, g * 128:(g + 1) * 128]

    c_uv.wait()
    vh = wuv.shape[2]
    for h in range(heads):
        oh = jnp.concatenate(
            [ol_s[g, pl.ds(h, bsz, stride=heads), :] for g in range(kvl // 128)], axis=1).astype(BF16)
        o_s[:, h * vh:(h + 1) * vh] = jnp.dot(oh, wuv_b[h], preferred_element_type=F32).astype(BF16)
    sq = jnp.zeros((bsz, 1), F32)
    for i in range(n_o):
        c_o[i].wait()
        cols = slice(i * oc, (i + 1) * oc)
        a = jnp.dot(o_s[...], wo_b[:, cols], preferred_element_type=F32)
        h1 = (x_ref[:, cols].astype(F32) + a).astype(BF16)
        h1_ref[:, cols] = h1
        h1 = h1.astype(F32)
        sq += jnp.sum(h1 * h1, axis=1, keepdims=True)
    u_ref[...] = (h1_ref[...].astype(F32) * lax.rsqrt(sq / hid + EPS)).astype(BF16)


def attention(n, x, cache, lens, ids, rw, w_q, w_dkv, w_uk, w_uv, w_o):
    bsz, hid = x.shape
    heads, nope, kvl = w_uk.shape
    l_max, kvd = cache.shape[1:]
    vm = pl.BlockSpec(memory_space=pltpu.VMEM)
    anys = pl.BlockSpec(memory_space=pl.ANY)
    cache_t = jnp.swapaxes(cache, 1, 2)
    rows = bsz * heads
    weights = (w_q, w_dkv.T, w_uk, w_uv, w_o, cache_t)
    row = jax.ShapeDtypeStruct((bsz, hid), BF16)
    return pl.pallas_call(
        attn_kernel,
        out_shape=(row, row, jax.ShapeDtypeStruct((bsz, kvd), BF16), jax.ShapeDtypeStruct((16, n * bsz), F32)),
        in_specs=[anys] * 11,
        out_specs=(vm,) * 4,
        scratch_shapes=[
            pltpu.VMEM(x.shape, BF16),
            pltpu.VMEM((1, bsz), jnp.int32),
            pltpu.SMEM((bsz,), jnp.int32),
            pltpu.VMEM(ids.shape[::-1], jnp.int32),
            pltpu.VMEM(rw.shape[::-1], F32),
        ] + [pltpu.VMEM(w.shape, BF16) for w in weights] + [
            pltpu.VMEM((bsz, w_q.shape[1]), BF16),
            pltpu.VMEM((kvl // 128, rows, 128), F32),
            pltpu.VMEM((rows, 128), F32),
            pltpu.VMEM((bsz, kvl + 128), F32),
            pltpu.VMEM((rows, l_max), F32),
            pltpu.VMEM((rows, l_max), BF16),
            pltpu.VMEM((kvl // 128, rows, 128), F32),
            pltpu.VMEM((bsz, w_o.shape[0]), BF16),
            pltpu.SemaphoreType.DMA((17,)),
        ],
        compiler_params=pltpu.CompilerParams(vmem_limit_bytes=60 << 20),
        cost_estimate=pl.CostEstimate(
            flops=2 * bsz * (hid * (w_q.shape[1] + kvd + w_o.shape[0]) + heads * kvl * (2 * nope + 2 * l_max)),
            bytes_accessed=2 * sum(w.size for w in weights), transcendentals=rows * l_max),
        name="attn",
    )(x, lens.reshape(1, bsz), lens, ids.T, rw.T, *weights)


def moe_kernel(n, cap, u_in, h1_in, meta_in, eg, eu, ed, sg, su, sd, y_ref,
               u_ref, h1_ref, meta_ref, wa, wb, meta_all, u_all, xr, act, disp, comb_t, comb, rows,
               pown, psend, precv, zsum, zrecv, sact,
               sem_i, sem_a, sem_b, ms, mr, us, ur, fs, fr, ps, pr, zs, zr):
    me = lax.axis_index('ep')
    nz = n // 2
    zi = me // 2
    co = lax.rem(me, 2)
    mate = zi * 2 + 1 - co
    b_dev, hid = u_ref.shape
    e_loc, _, inter = eg.shape
    slots = e_loc * cap
    n_tok = n * b_dev
    half = nz * b_dev
    n_ch = hid // CW

    def dev(d):
        return {'ep': d}

    def at_z(dz):
        return lax.rem(zi + dz, nz) * 2 + co

    def from_z(dz):
        return lax.rem(zi + nz - dz, nz)

    def a_copy(src, slot):
        return pltpu.make_async_copy(src, wa.at[slot], sem_a.at[slot])

    def start_down(j):
        slot = lax.rem(j, N_B)
        for e in range(e_loc):
            pltpu.make_async_copy(
                ed.at[e, :, pl.ds(pl.multiple_of(j * CW, CW), CW)],
                wb.at[slot, :, pl.ds(e * CW, CW)], sem_b.at[slot]).start()

    def wait_a(slot):
        a_copy(eg.at[0], slot).wait()

    def wait_b(slot):
        pltpu.make_async_copy(sd.at[pl.ds(0, inter)], wb.at[slot], sem_b.at[slot]).wait()

    n_gu = 2 * e_loc
    sh_a = [(sg, 0), (su, 0), (sg, 1), (su, 1)]

    def start_unit_a(i):
        slot = i % N_A
        if i < n_gu:
            a_copy((eg if i % 2 == 0 else eu).at[i // 2], slot).start()
        else:
            r, h = sh_a[i - n_gu]
            a_copy(r.at[:, pl.ds(h * inter, inter)], slot).start()

    small = [pltpu.make_async_copy(src, dst, sem_i.at[i]) for i, (src, dst) in enumerate(
        ((u_in, u_ref), (meta_in, meta_ref), (h1_in, h1_ref)))]
    for c in small:
        c.start()
    barrier = pltpu.get_barrier_semaphore()
    for d in range(1, n):
        pl.semaphore_signal(barrier, inc=1, device_id=dev(lax.rem(me + d, n)))
    for c in small:
        c.wait()
    pl.semaphore_wait(barrier, n - 1)

    def meta_copy(d):
        return pltpu.make_async_remote_copy(
            meta_ref, meta_all.at[me], ms.at[d - 1], mr.at[d - 1],
            device_id=dev(lax.rem(me + d, n)), device_id_type=pl.DeviceIdType.MESH)

    my_rows = pl.ds(pl.multiple_of(me * b_dev, b_dev), b_dev)

    def u_copy(k, target):
        return pltpu.make_async_remote_copy(
            u_ref, u_all.at[my_rows], us.at[k], ur.at[k],
            device_id=dev(target), device_id_type=pl.DeviceIdType.MESH)

    def fwd_copy(dz):
        blk = from_z(dz) * 2 + co
        r = u_all.at[pl.ds(pl.multiple_of(blk * b_dev, b_dev), b_dev)]
        return pltpu.make_async_remote_copy(
            r, r, fs.at[dz - 1], fr.at[dz - 1],
            device_id=dev(mate), device_id_type=pl.DeviceIdType.MESH)

    def recv_wait(dst, sem):
        pltpu.make_async_remote_copy(
            dst, dst, us.at[0], sem, device_id=dev(mate),
            device_id_type=pl.DeviceIdType.MESH).wait_recv()

    for d in range(1, n):
        meta_copy(d).start()
    for dz in (2, 1, 3):
        u_copy(dz - 1, at_z(dz)).start()
    u_copy(nz - 1, mate).start()
    for i in range(N_A):
        start_unit_a(i)
    for j in range(N_B):
        start_down(j)
    u_all[my_rows] = u_ref[...]

    tot = meta_ref[...]
    for d in range(1, n):
        src = lax.rem(me + n - d, n)
        recv_wait(meta_all.at[src], mr.at[d - 1])
        tot = tot + meta_all[src]
    half_m = tot.shape[0] // 2
    lane = lax.broadcasted_iota(jnp.int32, (e_loc, n_tok), 0) + (me * e_loc + 1)
    lane = lane.astype(F32)
    hit = jnp.zeros((e_loc, n_tok), F32)
    wt = jnp.zeros((e_loc, n_tok), F32)
    for k in range(half_m):
        eq = tot[k:k + 1] == lane
        hit = hit + jnp.where(eq, 1.0, 0.0)
        wt = wt + jnp.where(eq, tot[half_m + k:half_m + k + 1], 0.0)
    r0 = lax.broadcasted_iota(jnp.int32, (n_tok, n_tok), 0)
    r1 = lax.broadcasted_iota(jnp.int32, (n_tok, n_tok), 1)
    before = jnp.where(r0 < r1, 1.0, 0.0).astype(BF16)
    rank = jnp.dot(hit.astype(BF16), before, preferred_element_type=F32)
    rank = jnp.where(hit > 0.5, rank, -1.0)
    w1 = wt.astype(BF16).astype(F32)
    rest = wt - w1
    w2 = rest.astype(BF16).astype(F32)
    w3 = rest - w2
    row = lax.broadcasted_iota(jnp.int32, (cap, n_tok), 0).astype(F32)
    for e in range(e_loc):
        m = row == rank[e:e + 1]
        disp[e * cap:(e + 1) * cap] = jnp.where(m, 1.0, 0.0).astype(BF16)
        for p, w in enumerate((w1, w2, w3)):
            comb_t[p * slots + e * cap:p * slots + (e + 1) * cap] = jnp.where(m, w[e:e + 1], 0.0).astype(BF16)
    side = r0 // half
    blk = lax.rem(r0, half) // b_dev
    chip = lax.rem(blk + zi, nz)
    core = jnp.where(side == 0, co, 1 - co)
    tok = (chip * 2 + core) * b_dev + lax.rem(r0, b_dev)
    perm = jnp.where(r1 == tok, 1.0, 0.0).astype(BF16)
    comb[...] = lax.dot_general(perm, comb_t[...], (((1,), (1,)), ((), ())),
                                preferred_element_type=F32).astype(BF16)

    for dz in range(1, nz):
        blk_z = from_z(dz) * 2 + co
        recv_wait(u_all.at[pl.ds(pl.multiple_of(blk_z * b_dev, b_dev), b_dev)], ur.at[dz - 1])
        fwd_copy(dz).start()
    recv_wait(u_all.at[pl.ds(pl.multiple_of(mate * b_dev, b_dev), b_dev)], ur.at[nz - 1])
    for dz in range(1, nz):
        blk_z = from_z(dz) * 2 + 1 - co
        recv_wait(u_all.at[pl.ds(pl.multiple_of(blk_z * b_dev, b_dev), b_dev)], fr.at[dz - 1])

    @pl.loop(0, hid // 512)
    def _(i):
        cols = pl.ds(pl.multiple_of(i * 512, 512), 512)
        xr[:, cols] = jnp.dot(disp[...], u_all[:, cols], preferred_element_type=F32).astype(BF16)

    def gate_up(x, sa, sb, store):
        for c0 in range(0, inter, CW):
            c1 = min(c0 + CW, inter)
            g = jnp.dot(x, wa[sa, :, c0:c1], preferred_element_type=F32)
            v = jnp.dot(x, wa[sb, :, c0:c1], preferred_element_type=F32)
            store(c0, c1, (jax.nn.silu(g) * v).astype(BF16))

    def expert_body(e):
        sa = lax.rem(2 * e, N_A)
        sb = lax.rem(2 * e + 1, N_A)
        wait_a(sa)
        wait_a(sb)
        rs = pl.ds(pl.multiple_of(e * cap, cap), cap)

        def store(c0, c1, val):
            act[rs, c0:c1] = val

        gate_up(xr[rs, :], sa, sb, store)

    @pl.loop(0, e_loc)
    def _(e):
        expert_body(e)
        for t in range(2):
            i = 2 * e + t + N_A
            slot = lax.rem(i, N_A)

            @pl.when(jnp.logical_and(i < n_gu, lax.rem(i, 2) == 0))
            def _():
                a_copy(eg.at[lax.min(i // 2, e_loc - 1)], slot).start()

            @pl.when(jnp.logical_and(i < n_gu, lax.rem(i, 2) == 1))
            def _():
                a_copy(eu.at[lax.min(i // 2, e_loc - 1)], slot).start()

            for q in range(4):
                @pl.when(i == n_gu + q)
                def _():
                    r, h = sh_a[q]
                    a_copy(r.at[:, pl.ds(h * inter, inter)], slot).start()

    def p_copy(j):
        return pltpu.make_async_remote_copy(
            psend.at[j], precv.at[j], ps.at[j], pr.at[j],
            device_id=dev(mate), device_id_type=pl.DeviceIdType.MESH)

    def z_copy(j, dz):
        return pltpu.make_async_remote_copy(
            zsum.at[j, pl.ds(dz * b_dev, b_dev)], zrecv.at[j, dz - 1],
            zs.at[j, dz - 1], zr.at[j, dz - 1],
            device_id=dev(at_z(dz)), device_id_type=pl.DeviceIdType.MESH)

    def pass_on(j):
        recv_wait(precv.at[j], pr.at[j])
        zsum[j] = pown[j] + precv[j]
        for dz in range(1, nz):
            z_copy(j, dz).start()

    @pl.loop(0, n_ch)
    def _(j):
        slot = lax.rem(j, N_B)
        wait_b(slot)
        for e in range(e_loc):
            rows[e * cap:(e + 1) * cap] = jnp.dot(
                act[e * cap:(e + 1) * cap], wb[slot, :, e * CW:(e + 1) * CW],
                preferred_element_type=F32).astype(BF16)

        @pl.when(j + N_B < n_ch)
        def _():
            start_down(lax.min(j + N_B, n_ch - 1))

        for h in range(2):
            i = n_ch + h

            @pl.when(j + N_B == i)
            def _():
                pltpu.make_async_copy(sd.at[pl.ds(h * inter, inter)], wb.at[i % N_B], sem_b.at[i % N_B]).start()

        part = jnp.dot(comb[:, 0:slots], rows[...], preferred_element_type=F32)
        part += jnp.dot(comb[:, slots:2 * slots], rows[...], preferred_element_type=F32)
        part += jnp.dot(comb[:, 2 * slots:3 * slots], rows[...], preferred_element_type=F32)
        pown[j] = part[:half]
        psend[j] = part[half:]
        p_copy(j).start()

        @pl.when(j > 0)
        def _():
            pass_on(lax.max(j - 1, 0))

    for h in range(2):
        sa = (n_gu + 2 * h) % N_A
        sb = (n_gu + 2 * h + 1) % N_A
        wait_a(sa)
        wait_a(sb)

        def store(c0, c1, val):
            sact[:, h * inter + c0:h * inter + c1] = val

        gate_up(u_ref[...], sa, sb, store)
        if h == 0:
            pass_on(n_ch - 1)
    for h in range(2):
        wait_b((n_ch + h) % N_B)

    for j in range(n_ch):
        cols = slice(j * CW, (j + 1) * CW)
        s = jnp.dot(sact[:, :inter], wb[n_ch % N_B, :, cols], preferred_element_type=F32)
        s += jnp.dot(sact[:, inter:], wb[(n_ch + 1) % N_B, :, cols], preferred_element_type=F32)
        routed = zsum[j, :b_dev]
        for dz in range(1, nz):
            recv_wait(zrecv.at[j, dz - 1], zr.at[j, dz - 1])
            routed = routed + zrecv[j, dz - 1]
        y_ref[:, cols] = (h1_ref[:, cols].astype(F32) + s + routed).astype(BF16)

    for d in range(1, n):
        meta_copy(d).wait_send()
    for dz in range(1, nz):
        u_copy(dz - 1, at_z(dz)).wait_send()
        fwd_copy(dz).wait_send()
    u_copy(nz - 1, mate).wait_send()
    for j in range(n_ch):
        p_copy(j).wait_send()
        for dz in range(1, nz):
            z_copy(j, dz).wait_send()


def moe(n, u, h1, meta, eg, eu, ed, sg, su, sd, cap):
    b_dev, hid = u.shape
    e_loc, _, inter = eg.shape
    n_tok = n * b_dev
    slots = e_loc * cap
    nz = n // 2
    half = nz * b_dev
    n_ch = hid // CW
    dma = pltpu.SemaphoreType.DMA
    vm = pl.BlockSpec(memory_space=pltpu.VMEM)
    anys = pl.BlockSpec(memory_space=pl.ANY)
    flops = 2 * 3 * hid * inter * (slots + 2 * b_dev)
    return pl.pallas_call(
        functools.partial(moe_kernel, n, cap),
        out_shape=jax.ShapeDtypeStruct((b_dev, hid), BF16),
        in_specs=[anys] * 9,
        out_specs=vm,
        scratch_shapes=[
            pltpu.VMEM(u.shape, BF16),
            pltpu.VMEM(u.shape, BF16),
            pltpu.VMEM(meta.shape, F32),
            pltpu.VMEM((N_A, hid, inter), BF16),
            pltpu.VMEM((N_B, inter, hid), BF16),
            pltpu.VMEM((n,) + meta.shape, F32),
            pltpu.VMEM((n_tok, hid), BF16),
            pltpu.VMEM((slots, hid), BF16),
            pltpu.VMEM((slots, inter), BF16),
            pltpu.VMEM((slots, n_tok), BF16),
            pltpu.VMEM((3 * slots, n_tok), BF16),
            pltpu.VMEM((n_tok, 3 * slots), BF16),
            pltpu.VMEM((slots, CW), BF16),
            pltpu.VMEM((n_ch, half, CW), F32),
            pltpu.VMEM((n_ch, half, CW), F32),
            pltpu.VMEM((n_ch, half, CW), F32),
            pltpu.VMEM((n_ch, half, CW), F32),
            pltpu.VMEM((n_ch, nz - 1, b_dev, CW), F32),
            pltpu.VMEM((b_dev, 2 * inter), BF16),
            dma((3,)), dma((N_A,)), dma((N_B,)),
            dma((n - 1,)), dma((n - 1,)),
            dma((nz,)), dma((nz,)),
            dma((nz - 1,)), dma((nz - 1,)),
            dma((n_ch,)), dma((n_ch,)),
            dma((n_ch, nz - 1)), dma((n_ch, nz - 1)),
        ],
        compiler_params=pltpu.CompilerParams(
            collective_id=0, has_side_effects=True, vmem_limit_bytes=63 << 20),
        cost_estimate=pl.CostEstimate(flops=flops, bytes_accessed=30 * hid * inter * 2, transcendentals=0),
        name="moe",
    )(u, h1, meta, eg, eu, ed, sg, su, sd)


def solution(mesh):
    n = mesh.shape['ep']
    tok_spec = P(('rep', 'ep'))
    row_spec = P(('rep', 'ep'), None)
    cache_spec = P(('rep', 'ep'), None, None)
    exp_spec = P('ep', None, None)

    def local(x, cache, lens, ids, rw, w_q, w_dkv, w_uk, w_uv, w_o, s_gate, s_up, s_down, e_gate, e_up, e_down):
        b_dev, top = ids.shape
        e_loc = e_gate.shape[0]
        n_exp = e_loc * n
        cape = (CAP_FACTOR * b_dev * top + n_exp - 1) // n_exp
        h1, u, kv_new, meta = attention(n, x, cache, lens, ids, rw, w_q, w_dkv, w_uk, w_uv, w_o)
        y = moe(n, u, h1, meta, e_gate, e_up, e_down, s_gate, s_up, s_down, n * cape)
        return y, kv_new

    in_specs = (row_spec, cache_spec, tok_spec, row_spec, row_spec) + (P(),) * 8 + (exp_spec,) * 3
    return jax.shard_map(local, mesh=mesh, in_specs=in_specs, out_specs=(row_spec, row_spec), check_vma=False)
```

```python
import functools
import math

import jax
import jax.numpy as jnp
from jax import lax
from jax.experimental import pallas as pl
from jax.experimental.pallas import tpu as pltpu
from jax.sharding import PartitionSpec as P

EPS = 1e-6
ROPE_BASE = 1.0e4
CAP_FACTOR = 2
N_A = 5
N_B = 3
CW = 512
GW = 256
PER = 4
F32 = jnp.float32
BF16 = jnp.bfloat16


def attn_kernel(x_in, lrow_in, lens_in, ids_in, rw_in, wq, wdkv, wuk, wuv, wo, cache,
                h1_ref, u_ref, kvn_ref, meta_ref,
                x_ref, lrow_ref, lens_ref, ids_ref, rw_ref, wq_b, wdkv_b, wuk_b, wuv_b, wo_b, cache_b, q_a, a_s, q_s, ql_s, qr_s, kv_s, s_s, p_s, ol_s, o_s, sems):
    bsz, hid = x_in.shape
    heads, nope, kvl = wuk.shape
    kvd = wdkv.shape[0]
    rot = kvd - kvl
    l_max = cache.shape[2]
    qkd = nope + rot
    hh = hid // 2
    n_c = 4
    bc = bsz // n_c
    oh_dim = wo.shape[0] // 2
    copies = []

    def start(src, dst):
        c = pltpu.make_async_copy(src, dst, sems.at[len(copies)])
        c.start()
        copies.append(c)
        return c

    c_x = start(x_in, x_ref)
    c_small = [start(a, b) for a, b in ((lrow_in, lrow_ref), (lens_in, lens_ref), (ids_in, ids_ref), (rw_in, rw_ref))]
    c_q = [start(wq.at[i * hh:(i + 1) * hh], wq_b.at[i * hh:(i + 1) * hh]) for i in range(2)]
    c_kv = start(wdkv, wdkv_b)
    c_uk = start(wuk, wuk_b)
    c_c = [start(cache.at[i * bc:(i + 1) * bc], cache_b.at[i * bc:(i + 1) * bc]) for i in range(n_c)]
    c_uv = start(wuv, wuv_b)
    c_o = [start(wo.at[i * oh_dim:(i + 1) * oh_dim], wo_b.at[i * oh_dim:(i + 1) * oh_dim]) for i in range(2)]

    c_x.wait()
    for c in c_small:
        c.wait()

    me = lax.axis_index('ep')
    n_tok = meta_ref.shape[1]
    top = ids_ref.shape[0]
    lane = lax.broadcasted_iota(jnp.int32, (top, n_tok), 1) // bsz
    meta_ref[...] = jnp.zeros_like(meta_ref)
    for r, v in enumerate((ids_ref[...].astype(F32) + 1.0, rw_ref[...])):
        v = jnp.concatenate([v] * (n_tok // bsz), axis=1)
        meta_ref[r * 8:r * 8 + top] = jnp.where(lane == me, v, 0.0)

    eye = lax.broadcasted_iota(jnp.int32, (bsz, bsz), 0) == lax.broadcasted_iota(jnp.int32, (bsz, bsz), 1)
    pos = jnp.sum(jnp.where(eye, lrow_ref[...].astype(F32), 0.0), axis=1, keepdims=True)
    half = rot // 2
    li = lax.broadcasted_iota(jnp.int32, (bsz, rot), 1)
    fi = jnp.where(li < half, li, li - half).astype(F32)
    ang = pos * jnp.exp(fi * (-2.0 / rot * math.log(ROPE_BASE)))
    cs = jnp.cos(ang)
    sn = jnp.sin(ang)
    sn = jnp.where(li < half, -sn, sn)

    def rope(v):
        return v * cs + jnp.concatenate([v[:, half:], v[:, :half]], axis=1) * sn

    def norm(v):
        return v * lax.rsqrt(jnp.mean(v * v, axis=-1, keepdims=True) + EPS)

    xn = norm(x_ref[...].astype(F32)).astype(BF16)
    c_q[0].wait()
    q_a[...] = jnp.dot(xn[:, :hh], wq_b[:hh], preferred_element_type=F32)
    c_q[1].wait()
    q_s[...] = (q_a[...] + jnp.dot(xn[:, hh:], wq_b[hh:], preferred_element_type=F32)).astype(BF16)
    c_kv.wait()
    kv = lax.dot_general(xn, wdkv_b[...], (((1,), (1,)), ((), ())), preferred_element_type=F32)
    kvn_ref[:, :kvl] = norm(kv[:, :kvl]).astype(BF16)
    kvn_ref[:, kvl:] = rope(kv[:, kvl:]).astype(BF16)
    kv_s[:, :kvd] = kvn_ref[...].astype(F32)
    c_uk.wait()
    for h in range(heads):
        c0 = h * qkd
        rs = slice(h * bsz, (h + 1) * bsz)
        ql = jnp.dot(q_s[:, c0:c0 + nope], wuk_b[h], preferred_element_type=F32).astype(BF16).astype(F32)
        for g in range(kvl // 128):
            ql_s[g, rs] = ql[:, g * 128:(g + 1) * 128]
        qr_s[rs, :rot] = rope(q_s[:, c0 + nope:c0 + qkd].astype(F32)).astype(BF16).astype(F32)

    col = lax.broadcasted_iota(jnp.int32, (heads, l_max), 1)
    scale = qkd ** -0.5
    unroll = 8
    for i in range(n_c):
        c_c[i].wait()

        @pl.loop(0, bc // unroll)
        def _(t):
            for k in range(unroll):
                b = i * bc + t * unroll + k
                ql = jnp.concatenate(
                    [ql_s[g, pl.ds(b, heads, stride=bsz), :] for g in range(kvl // 128)], axis=1)
                qr = qr_s[pl.ds(b, heads, stride=bsz), :][:, :rot]
                kl = kv_s[pl.ds(b, 1), :]
                s = jnp.dot(ql.astype(BF16), cache_b[b, :kvl], preferred_element_type=F32)
                s += jnp.dot(qr.astype(BF16), cache_b[b, kvl:], preferred_element_type=F32)
                s_new = jnp.sum(ql * kl[:, :kvl], axis=1, keepdims=True)
                s_new += jnp.sum(qr * kl[:, kvl:kvd], axis=1, keepdims=True)
                n_live = lens_ref[b]
                s = jnp.where(col < n_live, s, jnp.where(col == n_live, s_new, -jnp.inf)) * scale
                s_s[pl.ds(pl.multiple_of(b * heads, heads), heads)] = s

    blk = 128

    @pl.loop(0, bsz * heads // blk)
    def _(t):
        rs = pl.ds(pl.multiple_of(t * blk, blk), blk)
        s = s_s[rs]
        e = jnp.exp(s - jnp.max(s, axis=1, keepdims=True))
        p_s[rs] = (e / jnp.sum(e, axis=1, keepdims=True)).astype(BF16)

    @pl.loop(0, bsz // unroll)
    def _(t):
        for k in range(unroll):
            b = t * unroll + k
            rs = pl.ds(pl.multiple_of(b * heads, heads), heads)
            n_live = lens_ref[b]
            p = p_s[rs].astype(F32)
            p_old = jnp.where(col < n_live, p, 0.0).astype(BF16)
            p_new = jnp.sum(jnp.where(col == n_live, p, 0.0), axis=1, keepdims=True)
            o = lax.dot_general(p_old, cache_b[b, :kvl], (((1,), (1,)), ((), ())), preferred_element_type=F32)
            o += p_new * kv_s[pl.ds(b, 1), :][:, :kvl]
            o = o.astype(BF16).astype(F32)
            for g in range(kvl // 128):
                ol_s[g, rs] = o[:, g * 128:(g + 1) * 128]

    c_uv.wait()
    vh = wuv.shape[2]
    for h in range(heads):
        oh = jnp.concatenate(
            [ol_s[g, pl.ds(h, bsz, stride=heads), :] for g in range(kvl // 128)], axis=1).astype(BF16)
        o_s[:, h * vh:(h + 1) * vh] = jnp.dot(oh, wuv_b[h], preferred_element_type=F32).astype(BF16)
    c_o[0].wait()
    a_s[...] = jnp.dot(o_s[:, :oh_dim], wo_b[:oh_dim], preferred_element_type=F32)
    c_o[1].wait()
    a = a_s[...] + jnp.dot(o_s[:, oh_dim:], wo_b[oh_dim:], preferred_element_type=F32)
    h1_ref[...] = (x_ref[...].astype(F32) + a).astype(BF16)
    h1 = h1_ref[...].astype(F32)
    sq = jnp.sum(h1 * h1, axis=1, keepdims=True)
    u_ref[...] = (h1_ref[...].astype(F32) * lax.rsqrt(sq / hid + EPS)).astype(BF16)


def attention(n, x, cache, lens, ids, rw, w_q, w_dkv, w_uk, w_uv, w_o):
    bsz, hid = x.shape
    heads, nope, kvl = w_uk.shape
    l_max, kvd = cache.shape[1:]
    vm = pl.BlockSpec(memory_space=pltpu.VMEM)
    anys = pl.BlockSpec(memory_space=pl.ANY)
    cache_t = jnp.swapaxes(cache, 1, 2)
    rows = bsz * heads
    weights = (w_q, w_dkv.T, w_uk, w_uv, w_o, cache_t)
    row = jax.ShapeDtypeStruct((bsz, hid), BF16)
    return pl.pallas_call(
        attn_kernel,
        out_shape=(row, row, jax.ShapeDtypeStruct((bsz, kvd), BF16), jax.ShapeDtypeStruct((16, n * bsz), F32)),
        in_specs=[anys] * 11,
        out_specs=(vm,) * 4,
        scratch_shapes=[
            pltpu.VMEM(x.shape, BF16),
            pltpu.VMEM((1, bsz), jnp.int32),
            pltpu.SMEM((bsz,), jnp.int32),
            pltpu.VMEM(ids.shape[::-1], jnp.int32),
            pltpu.VMEM(rw.shape[::-1], F32),
        ] + [pltpu.VMEM(w.shape, BF16) for w in weights] + [
            pltpu.VMEM((bsz, w_q.shape[1]), F32),
            pltpu.VMEM((bsz, hid), F32),
            pltpu.VMEM((bsz, w_q.shape[1]), BF16),
            pltpu.VMEM((kvl // 128, rows, 128), F32),
            pltpu.VMEM((rows, 128), F32),
            pltpu.VMEM((bsz, kvl + 128), F32),
            pltpu.VMEM((rows, l_max), F32),
            pltpu.VMEM((rows, l_max), BF16),
            pltpu.VMEM((kvl // 128, rows, 128), F32),
            pltpu.VMEM((bsz, w_o.shape[0]), BF16),
            pltpu.SemaphoreType.DMA((17,)),
        ],
        compiler_params=pltpu.CompilerParams(vmem_limit_bytes=60 << 20),
        cost_estimate=pl.CostEstimate(
            flops=2 * bsz * (hid * (w_q.shape[1] + kvd + w_o.shape[0]) + heads * kvl * (2 * nope + 2 * l_max)),
            bytes_accessed=2 * sum(w.size for w in weights), transcendentals=rows * l_max),
        name="attn",
    )(x, lens.reshape(1, bsz), lens, ids.T, rw.T, *weights)


def moe_kernel(n, cap, u_in, h1_in, meta_in, eg, eu, ed, sg, su, sd, y_ref,
               u_ref, h1_ref, meta_ref, wa, wb, meta_all, u_all, xr, act, disp, comb_t, comb, rows,
               pown, psend, precv, zsum, zrecv, sact,
               sem_i, sem_a, sem_b, ms, mr, us, ur, fs, fr, ps, pr, zs, zr):
    me = lax.axis_index('ep')
    nz = n // 2
    zi = me // 2
    co = lax.rem(me, 2)
    mate = zi * 2 + 1 - co
    b_dev, hid = u_ref.shape
    e_loc, _, inter = eg.shape
    slots = e_loc * cap
    n_tok = n * b_dev
    half = nz * b_dev
    n_ch = hid // CW

    def dev(d):
        return {'ep': d}

    def at_z(dz):
        return lax.rem(zi + dz, nz) * 2 + co

    def from_z(dz):
        return lax.rem(zi + nz - dz, nz)

    def a_copy(src, slot):
        return pltpu.make_async_copy(src, wa.at[slot], sem_a.at[slot])

    parts = e_loc // PER
    n_st = n_ch * parts

    def start_down(t):
        slot = lax.rem(t, N_B)
        j = t // parts
        first = lax.rem(t, parts) * PER
        for e in range(PER):
            pltpu.make_async_copy(
                ed.at[first + e, :, pl.ds(pl.multiple_of(j * CW, CW), CW)],
                wb.at[slot, :, pl.ds(e * CW, CW)], sem_b.at[slot]).start()

    def wait_a(slot):
        a_copy(eg.at[0], slot).wait()

    def wait_b(slot):
        pltpu.make_async_copy(sd.at[pl.ds(0, inter)], wb.at[slot], sem_b.at[slot]).wait()

    n_gu = 2 * e_loc
    sh_a = [(sg, 0), (su, 0), (sg, 1), (su, 1)]

    def start_unit_a(i):
        slot = i % N_A
        if i < n_gu:
            a_copy((eg if i % 2 == 0 else eu).at[i // 2], slot).start()
        else:
            r, h = sh_a[i - n_gu]
            a_copy(r.at[:, pl.ds(h * inter, inter)], slot).start()

    small = [pltpu.make_async_copy(src, dst, sem_i.at[i]) for i, (src, dst) in enumerate(
        ((u_in, u_ref), (meta_in, meta_ref), (h1_in, h1_ref)))]
    for c in small:
        c.start()
    barrier = pltpu.get_barrier_semaphore()
    for d in range(1, n):
        pl.semaphore_signal(barrier, inc=1, device_id=dev(lax.rem(me + d, n)))
    for c in small:
        c.wait()
    pl.semaphore_wait(barrier, n - 1)

    def meta_copy(d):
        return pltpu.make_async_remote_copy(
            meta_ref, meta_all.at[me], ms.at[d - 1], mr.at[d - 1],
            device_id=dev(lax.rem(me + d, n)), device_id_type=pl.DeviceIdType.MESH)

    my_rows = pl.ds(pl.multiple_of(me * b_dev, b_dev), b_dev)

    def u_copy(k, target):
        return pltpu.make_async_remote_copy(
            u_ref, u_all.at[my_rows], us.at[k], ur.at[k],
            device_id=dev(target), device_id_type=pl.DeviceIdType.MESH)

    def fwd_copy(dz):
        blk = from_z(dz) * 2 + co
        r = u_all.at[pl.ds(pl.multiple_of(blk * b_dev, b_dev), b_dev)]
        return pltpu.make_async_remote_copy(
            r, r, fs.at[dz - 1], fr.at[dz - 1],
            device_id=dev(mate), device_id_type=pl.DeviceIdType.MESH)

    def recv_wait(dst, sem):
        pltpu.make_async_remote_copy(
            dst, dst, us.at[0], sem, device_id=dev(mate),
            device_id_type=pl.DeviceIdType.MESH).wait_recv()

    for d in range(1, n):
        meta_copy(d).start()
    for dz in (2, 1, 3):
        u_copy(dz - 1, at_z(dz)).start()
    u_copy(nz - 1, mate).start()
    for i in range(N_A):
        start_unit_a(i)
    for j in range(N_B):
        start_down(j)
    u_all[my_rows] = u_ref[...]

    tot = meta_ref[...]
    for d in range(1, n):
        src = lax.rem(me + n - d, n)
        recv_wait(meta_all.at[src], mr.at[d - 1])
        tot = tot + meta_all[src]
    half_m = tot.shape[0] // 2
    lane = lax.broadcasted_iota(jnp.int32, (e_loc, n_tok), 0) + (me * e_loc + 1)
    lane = lane.astype(F32)
    hit = jnp.zeros((e_loc, n_tok), F32)
    wt = jnp.zeros((e_loc, n_tok), F32)
    for k in range(half_m):
        eq = tot[k:k + 1] == lane
        hit = hit + jnp.where(eq, 1.0, 0.0)
        wt = wt + jnp.where(eq, tot[half_m + k:half_m + k + 1], 0.0)
    r0 = lax.broadcasted_iota(jnp.int32, (n_tok, n_tok), 0)
    r1 = lax.broadcasted_iota(jnp.int32, (n_tok, n_tok), 1)
    before = jnp.where(r0 < r1, 1.0, 0.0).astype(BF16)
    rank = jnp.dot(hit.astype(BF16), before, preferred_element_type=F32)
    rank = jnp.where(hit > 0.5, rank, -1.0)
    w1 = wt.astype(BF16).astype(F32)
    rest = wt - w1
    w2 = rest.astype(BF16).astype(F32)
    w3 = rest - w2
    row = lax.broadcasted_iota(jnp.int32, (cap, n_tok), 0).astype(F32)
    for e in range(e_loc):
        m = row == rank[e:e + 1]
        disp[e * cap:(e + 1) * cap] = jnp.where(m, 1.0, 0.0).astype(BF16)
        for p, w in enumerate((w1, w2, w3)):
            comb_t[p * slots + e * cap:p * slots + (e + 1) * cap] = jnp.where(m, w[e:e + 1], 0.0).astype(BF16)
    side = r0 // half
    blk = lax.rem(r0, half) // b_dev
    chip = lax.rem(blk + zi, nz)
    core = jnp.where(side == 0, co, 1 - co)
    tok = (chip * 2 + core) * b_dev + lax.rem(r0, b_dev)
    perm = jnp.where(r1 == tok, 1.0, 0.0).astype(BF16)
    comb[...] = lax.dot_general(perm, comb_t[...], (((1,), (1,)), ((), ())),
                                preferred_element_type=F32).astype(BF16)

    for dz in range(1, nz):
        blk_z = from_z(dz) * 2 + co
        recv_wait(u_all.at[pl.ds(pl.multiple_of(blk_z * b_dev, b_dev), b_dev)], ur.at[dz - 1])
        fwd_copy(dz).start()
    recv_wait(u_all.at[pl.ds(pl.multiple_of(mate * b_dev, b_dev), b_dev)], ur.at[nz - 1])
    for dz in range(1, nz):
        blk_z = from_z(dz) * 2 + 1 - co
        recv_wait(u_all.at[pl.ds(pl.multiple_of(blk_z * b_dev, b_dev), b_dev)], fr.at[dz - 1])

    @pl.loop(0, hid // 512)
    def _(i):
        cols = pl.ds(pl.multiple_of(i * 512, 512), 512)
        xr[:, cols] = jnp.dot(disp[...], u_all[:, cols], preferred_element_type=F32).astype(BF16)

    def gate_up(x, sa, sb, store):
        for c0 in range(0, inter, GW):
            c1 = min(c0 + GW, inter)
            g = jnp.dot(x, wa[sa, :, c0:c1], preferred_element_type=F32)
            v = jnp.dot(x, wa[sb, :, c0:c1], preferred_element_type=F32)
            store(c0, c1, (jax.nn.silu(g) * v).astype(BF16))

    def expert_body(e):
        sa = lax.rem(2 * e, N_A)
        sb = lax.rem(2 * e + 1, N_A)
        wait_a(sa)
        wait_a(sb)
        rs = pl.ds(pl.multiple_of(e * cap, cap), cap)

        def store(c0, c1, val):
            act[rs, c0:c1] = val

        gate_up(xr[rs, :], sa, sb, store)

    @pl.loop(0, e_loc)
    def _(e):
        expert_body(e)
        for t in range(2):
            i = 2 * e + t + N_A
            slot = lax.rem(i, N_A)

            @pl.when(jnp.logical_and(i < n_gu, lax.rem(i, 2) == 0))
            def _():
                a_copy(eg.at[lax.min(i // 2, e_loc - 1)], slot).start()

            @pl.when(jnp.logical_and(i < n_gu, lax.rem(i, 2) == 1))
            def _():
                a_copy(eu.at[lax.min(i // 2, e_loc - 1)], slot).start()

            for q in range(4):
                @pl.when(i == n_gu + q)
                def _():
                    r, h = sh_a[q]
                    a_copy(r.at[:, pl.ds(h * inter, inter)], slot).start()

    def p_copy(j):
        return pltpu.make_async_remote_copy(
            psend.at[j], precv.at[j], ps.at[j], pr.at[j],
            device_id=dev(mate), device_id_type=pl.DeviceIdType.MESH)

    def z_copy(j, dz):
        return pltpu.make_async_remote_copy(
            zsum.at[j, pl.ds(dz * b_dev, b_dev)], zrecv.at[j, dz - 1],
            zs.at[j, dz - 1], zr.at[j, dz - 1],
            device_id=dev(at_z(dz)), device_id_type=pl.DeviceIdType.MESH)

    def pass_on(j):
        recv_wait(precv.at[j], pr.at[j])
        zsum[j] = pown[j] + precv[j]
        for dz in range(1, nz):
            z_copy(j, dz).start()

    @pl.loop(0, n_st)
    def _(t):
        slot = lax.rem(t, N_B)
        j = t // parts
        first = lax.rem(t, parts) * PER * cap
        wait_b(slot)
        for e in range(PER):
            rs = pl.ds(pl.multiple_of(first + e * cap, cap), cap)
            rows[rs] = jnp.dot(
                act[rs], wb[slot, :, e * CW:(e + 1) * CW], preferred_element_type=F32).astype(BF16)

        @pl.when(t + N_B < n_st)
        def _():
            start_down(lax.min(t + N_B, n_st - 1))

        for h in range(2):
            i = n_st + h

            @pl.when(t + N_B == i)
            def _():
                pltpu.make_async_copy(sd.at[pl.ds(h * inter, inter)], wb.at[i % N_B], sem_b.at[i % N_B]).start()

        @pl.when(lax.rem(t, parts) == parts - 1)
        def _():
            part = jnp.dot(comb[:, 0:slots], rows[...], preferred_element_type=F32)
            part += jnp.dot(comb[:, slots:2 * slots], rows[...], preferred_element_type=F32)
            part += jnp.dot(comb[:, 2 * slots:3 * slots], rows[...], preferred_element_type=F32)
            pown[j] = part[:half]
            psend[j] = part[half:]
            p_copy(j).start()

        @pl.when(jnp.logical_and(lax.rem(t, parts) == 0, t > 0))
        def _():
            pass_on(lax.max(j - 1, 0))

    for h in range(2):
        sa = (n_gu + 2 * h) % N_A
        sb = (n_gu + 2 * h + 1) % N_A
        wait_a(sa)
        wait_a(sb)

        def store(c0, c1, val):
            sact[:, h * inter + c0:h * inter + c1] = val

        if h == 0:
            pass_on(n_ch - 1)
        gate_up(u_ref[...], sa, sb, store)
    for h in range(2):
        wait_b((n_st + h) % N_B)

    for j in range(n_ch):
        cols = slice(j * CW, (j + 1) * CW)
        s = jnp.dot(sact[:, :inter], wb[n_st % N_B, :, cols], preferred_element_type=F32)
        s += jnp.dot(sact[:, inter:], wb[(n_st + 1) % N_B, :, cols], preferred_element_type=F32)
        routed = zsum[j, :b_dev]
        for dz in range(1, nz):
            recv_wait(zrecv.at[j, dz - 1], zr.at[j, dz - 1])
            routed = routed + zrecv[j, dz - 1]
        y_ref[:, cols] = (h1_ref[:, cols].astype(F32) + s + routed).astype(BF16)

    for d in range(1, n):
        meta_copy(d).wait_send()
    for dz in range(1, nz):
        u_copy(dz - 1, at_z(dz)).wait_send()
        fwd_copy(dz).wait_send()
    u_copy(nz - 1, mate).wait_send()
    for j in range(n_ch):
        p_copy(j).wait_send()
        for dz in range(1, nz):
            z_copy(j, dz).wait_send()


def moe(n, u, h1, meta, eg, eu, ed, sg, su, sd, cap):
    b_dev, hid = u.shape
    e_loc, _, inter = eg.shape
    n_tok = n * b_dev
    slots = e_loc * cap
    nz = n // 2
    half = nz * b_dev
    n_ch = hid // CW
    dma = pltpu.SemaphoreType.DMA
    vm = pl.BlockSpec(memory_space=pltpu.VMEM)
    anys = pl.BlockSpec(memory_space=pl.ANY)
    flops = 2 * 3 * hid * inter * (slots + 2 * b_dev)
    return pl.pallas_call(
        functools.partial(moe_kernel, n, cap),
        out_shape=jax.ShapeDtypeStruct((b_dev, hid), BF16),
        in_specs=[anys] * 9,
        out_specs=vm,
        scratch_shapes=[
            pltpu.VMEM(u.shape, BF16),
            pltpu.VMEM(u.shape, BF16),
            pltpu.VMEM(meta.shape, F32),
            pltpu.VMEM((N_A, hid, inter), BF16),
            pltpu.VMEM((N_B, inter, hid), BF16),
            pltpu.VMEM((n,) + meta.shape, F32),
            pltpu.VMEM((n_tok, hid), BF16),
            pltpu.VMEM((slots, hid), BF16),
            pltpu.VMEM((slots, inter), BF16),
            pltpu.VMEM((slots, n_tok), BF16),
            pltpu.VMEM((3 * slots, n_tok), BF16),
            pltpu.VMEM((n_tok, 3 * slots), BF16),
            pltpu.VMEM((slots, CW), BF16),
            pltpu.VMEM((n_ch, half, CW), F32),
            pltpu.VMEM((n_ch, half, CW), F32),
            pltpu.VMEM((n_ch, half, CW), F32),
            pltpu.VMEM((n_ch, half, CW), F32),
            pltpu.VMEM((n_ch, nz - 1, b_dev, CW), F32),
            pltpu.VMEM((b_dev, 2 * inter), BF16),
            dma((3,)), dma((N_A,)), dma((N_B,)),
            dma((n - 1,)), dma((n - 1,)),
            dma((nz,)), dma((nz,)),
            dma((nz - 1,)), dma((nz - 1,)),
            dma((n_ch,)), dma((n_ch,)),
            dma((n_ch, nz - 1)), dma((n_ch, nz - 1)),
        ],
        compiler_params=pltpu.CompilerParams(
            collective_id=0, has_side_effects=True, vmem_limit_bytes=63 << 20),
        cost_estimate=pl.CostEstimate(flops=flops, bytes_accessed=30 * hid * inter * 2, transcendentals=0),
        name="moe",
    )(u, h1, meta, eg, eu, ed, sg, su, sd)


def solution(mesh):
    n = mesh.shape['ep']
    tok_spec = P(('rep', 'ep'))
    row_spec = P(('rep', 'ep'), None)
    cache_spec = P(('rep', 'ep'), None, None)
    exp_spec = P('ep', None, None)

    def local(x, cache, lens, ids, rw, w_q, w_dkv, w_uk, w_uv, w_o, s_gate, s_up, s_down, e_gate, e_up, e_down):
        b_dev, top = ids.shape
        e_loc = e_gate.shape[0]
        n_exp = e_loc * n
        cape = (CAP_FACTOR * b_dev * top + n_exp - 1) // n_exp
        h1, u, kv_new, meta = attention(n, x, cache, lens, ids, rw, w_q, w_dkv, w_uk, w_uv, w_o)
        y = moe(n, u, h1, meta, e_gate, e_up, e_down, s_gate, s_up, s_down, n * cape)
        return y, kv_new

    in_specs = (row_spec, cache_spec, tok_spec, row_spec, row_spec) + (P(),) * 8 + (exp_spec,) * 3
    return jax.shard_map(local, mesh=mesh, in_specs=in_specs, out_specs=(row_spec, row_spec), check_vma=False)
```
